32 devices in a mesh: section: 4 (over y, x), dp: 8 (over z, core).
Axes of the slice: x: 2, y: 2, z: 4, core: 2. Of those that a mesh axis runs over, the one named last changes fastest.
Arguments:
- inputs: bfloat16 [4, 2, 512, 4096], P('section', None, 'dp'), may hold values from -6 to 6
- cotangent: bfloat16 [2, 512, 4096], P(None, 'dp'), may hold values from -6 to 6
- norm_gain: bfloat16 [4, 4096], P('section', 'dp'), may hold values from 0.5 to 1.5
- key_weight: bfloat16 [4, 4096, 512], P('section', 'dp'), may hold values from -0.09375 to 0.09375
- value_weight: bfloat16 [4, 4096, 512], P('section', 'dp'), may hold values from -0.09375 to 0.09375
- plan: int32 [4, 2], P('section'), may hold values from 0 to 1, each once within a row
Outputs:
- grad_inputs: bfloat16 [4, 2, 512, 4096], P('section', None, 'dp')
- key_weight_grad: float32 [4, 4096, 512], P('section', 'dp')
- value_weight_grad: float32 [4, 4096, 512], P('section', 'dp')
- gain_grad: float32 [4, 4096], P('section', 'dp')
The draws below stay inside these ranges and needn't reach their ends.
Inputs may be any that keep to these rules, and one draw needn't show every extreme that they name: Each row of plan lists every micro-batch once.
All inputs are finite; a program needn't handle non-finite values.
Results may differ from the reference program's by a relative error of at most 0.03.
Values may be sent and summed in bfloat16 or wider, within the bound.
A program may use at most 128 MiB of HBM per device.

```python
import math
import jax
import jax.numpy as jnp
from jax import lax

D = 4096
HEADS = 32
KV_HEADS = 4
HEAD_DIM = 128
KV = 512
GROUP = 8
MB = 2
TOK_DEV = 64
TOKENS = 512
N_SECTION = 4
N_DP = 8


def strengthened(drawn, stream_key, source, target, blocks, factor):
    def block_of(position):
        return (jnp.arange(drawn.shape[position]) // (drawn.shape[position] // blocks)).reshape((-1,) + (1,) * (drawn.ndim - 1 - position))

    near = jax.random.permutation(stream_key, blocks)[block_of(target)]
    second = (block_of(target) + blocks // 2) % blocks
    return jnp.where((block_of(source) == near) | (block_of(source) == second), factor * drawn, drawn)


def level_of(key, shape, cuts, low, largest):
    level = 1.0
    for position, blocks in cuts:
        heights = jax.random.uniform(jax.random.fold_in(jax.random.fold_in(key, 6), position), (blocks,), jnp.float32, low / len(cuts), largest / len(cuts))
        level = level * jnp.repeat(jnp.exp(heights), shape[position] // blocks).reshape((-1,) + (1,) * (len(shape) - 1 - position))
    return level


def normal_values(stream_key, dims, scale, limit, split=(), held_as=jnp.bfloat16):
    entries = scale * jax.random.normal(stream_key, dims, jnp.float32)
    if split:
        entries = entries * level_of(stream_key, dims, split, -0.22, 0.18)
    return jnp.clip(entries, -limit, limit).astype(held_as)


def noise_with(stream_key, extent, spread, most, split, heavy, kind=jnp.bfloat16):
    result = spread * jax.random.normal(stream_key, extent, jnp.float32)
    if split:
        result = result * level_of(stream_key, extent, split, -0.22, 0.18)
    return jnp.clip(strengthened(result, jax.random.fold_in(stream_key, 3), *heavy), -most, most).astype(kind)


def setup_inputs(seed: int = 0) -> dict:
    splits = jax.random.split(jax.random.key(seed), 7)
    return {
        "inputs": noise_with(splits[0], (N_SECTION, MB, TOKENS, D), 1.0, 6.0, ((0, 4), (2, 8)), (2, 3, 8, 2.0)),
        "cotangent": normal_values(splits[1], (MB, TOKENS, D), 1.0, 6.0, ((1, 8),)),
        "norm_gain": jnp.clip(1.0 + 0.1 * jax.random.normal(splits[2], (N_SECTION, D), jnp.float32), 0.5, 1.5).astype(jnp.bfloat16),
        "key_weight": normal_values(splits[3], (N_SECTION, D, KV), D ** -0.5, 0.09375, ((0, 4), (1, 8))),
        "value_weight": normal_values(splits[4], (N_SECTION, D, KV), D ** -0.5, 0.09375, ((0, 4), (1, 8))),
        "plan": jax.vmap(lambda own: jax.random.permutation(own, MB))(jax.random.split(splits[5], N_SECTION)).reshape((N_SECTION, MB)).astype(jnp.int32),
    }


eps = 1e-05
rope_base = 500000.0

def rope_tables(length, head_dim):
    half_dim = head_dim // 2
    frequency = rope_base ** (-(jnp.arange(half_dim, dtype=jnp.float32) * 2.0 / head_dim))
    angles = jnp.arange(length, dtype=jnp.float32)[:, None] * frequency[None, :]
    cosine = jnp.concatenate([jnp.cos(angles), jnp.cos(angles)], axis=-1)
    sine_tab = jnp.concatenate([jnp.sin(angles), jnp.sin(angles)], axis=-1)
    return (cosine[:, None, :], sine_tab[:, None, :])

def turned(values):
    half_dim = values.shape[-1] // 2
    return jnp.concatenate([-values[..., half_dim:], values[..., :half_dim]], axis=-1)

def rotate(values, cosine, sine_tab):
    return values * cosine + turned(values) * sine_tab

def unrotate(values, cosine, sine_tab):
    return values * cosine - turned(values) * sine_tab

def forward(x_rows, gain, w_key, w_value):
    batch_count = x_rows.shape[0]
    length = x_rows.shape[1]
    score_scale = 1.0 / math.sqrt(HEAD_DIM)
    widened = x_rows.astype(jnp.float32)
    inv_rms = lax.rsqrt(lax.optimization_barrier(jnp.mean(widened * widened, axis=-1, keepdims=True)) + eps)
    gain_full = gain.astype(jnp.float32)
    normed = (widened * inv_rms * gain_full).astype(jnp.bfloat16)
    flat_normed = normed.reshape(batch_count * length, D)
    key_pre = jnp.dot(flat_normed, w_key, preferred_element_type=jnp.float32).reshape(batch_count, length, KV_HEADS, HEAD_DIM)
    value_heads = jnp.dot(flat_normed, w_value, preferred_element_type=jnp.float32).astype(jnp.bfloat16).reshape(batch_count, length, KV_HEADS, HEAD_DIM)
    cosine, sine_tab = rope_tables(length, HEAD_DIM)
    key_rot = rotate(key_pre, cosine, sine_tab).astype(jnp.bfloat16)
    query_rot = rotate(normed.astype(jnp.float32).reshape(batch_count, length, HEADS, HEAD_DIM), cosine, sine_tab).astype(jnp.bfloat16)
    query_rot = query_rot.reshape(batch_count, length, KV_HEADS, GROUP, HEAD_DIM)
    scores = jnp.einsum('blkgd,bmkd->bkglm', query_rot.astype(jnp.float32), key_rot.astype(jnp.float32)) * score_scale
    causal = jnp.arange(length)[:, None] >= jnp.arange(length)[None, :]
    raised = jnp.where(causal, jnp.exp(scores), 0.0)
    attn_prob = raised / lax.optimization_barrier(jnp.sum(raised, axis=-1, keepdims=True))
    prob_low = attn_prob.astype(jnp.bfloat16)
    return (widened, inv_rms, normed, query_rot, key_rot, value_heads, attn_prob, prob_low)

def backward(upper_grad, widened, inv_rms, normed, query_rot, key_rot, value_heads, attn_prob, prob_low, gain, w_key, w_value):
    batch_count = upper_grad.shape[0]
    length = upper_grad.shape[1]
    score_scale = 1.0 / math.sqrt(HEAD_DIM)
    grad_heads = upper_grad.astype(jnp.float32).reshape(batch_count, length, KV_HEADS, GROUP, HEAD_DIM)
    grad_prob = jnp.einsum('blkgd,bmkd->bkglm', grad_heads, value_heads.astype(jnp.float32))
    grad_value = jnp.einsum('bkglm,blkgd->bmkd', prob_low.astype(jnp.float32), grad_heads).astype(jnp.bfloat16)
    row_dot = lax.optimization_barrier(jnp.sum(attn_prob * grad_prob, axis=-1, keepdims=True))
    grad_score = (attn_prob * (grad_prob - row_dot) * score_scale).astype(jnp.bfloat16)
    grad_query = jnp.einsum('bkglm,bmkd->blkgd', grad_score.astype(jnp.float32), key_rot.astype(jnp.float32))
    grad_key = jnp.einsum('bkglm,blkgd->bmkd', grad_score.astype(jnp.float32), query_rot.astype(jnp.float32))
    cosine, sine_tab = rope_tables(length, HEAD_DIM)
    query_back = unrotate(grad_query.reshape(batch_count, length, HEADS, HEAD_DIM), cosine, sine_tab).reshape(batch_count, length, D)
    key_back = unrotate(grad_key, cosine, sine_tab).astype(jnp.bfloat16).reshape(batch_count * length, KV)
    value_flat = grad_value.reshape(batch_count * length, KV)
    projected_back = jnp.dot(key_back, w_key.T, preferred_element_type=jnp.float32) + jnp.dot(value_flat, w_value.T, preferred_element_type=jnp.float32)
    grad_normed = query_back + projected_back.reshape(batch_count, length, D)
    gain_full = gain.astype(jnp.float32)
    gain_term = grad_normed * widened * inv_rms
    projected = lax.optimization_barrier(jnp.mean(gain_term * gain_full, axis=-1, keepdims=True))
    lower_grad = upper_grad.astype(jnp.float32) + inv_rms * gain_full * grad_normed - widened * inv_rms * inv_rms * projected
    return (lower_grad.astype(jnp.bfloat16), key_back, value_flat, gain_term)

def regroup(array):
    return array.reshape(MB, N_DP, TOK_DEV, -1).transpose(1, 0, 2, 3).reshape(N_DP, MB * TOK_DEV, -1)

def add_group(totals, pieces):
    normed, key_back, value_flat, gain_term = pieces
    sum_key = jnp.dot(normed.T, key_back, preferred_element_type=jnp.float32)
    sum_value = jnp.dot(normed.T, value_flat, preferred_element_type=jnp.float32)
    sum_gain = lax.optimization_barrier(jnp.sum(gain_term, axis=0))
    rounded_key = lax.optimization_barrier(sum_key.astype(jnp.bfloat16)).astype(jnp.float32)
    rounded_value = lax.optimization_barrier(sum_value.astype(jnp.bfloat16)).astype(jnp.float32)
    rounded_gain = lax.optimization_barrier(sum_gain.astype(jnp.bfloat16)).astype(jnp.float32)
    return ((totals[0] + rounded_key, totals[1] + rounded_value, totals[2] + rounded_gain), None)

def reference(inputs, cotangent, norm_gain, key_weight, value_weight, plan):
    upper_grad = cotangent.reshape(MB * N_DP, TOK_DEV, D)
    grad_list = [None] * N_SECTION
    key_list = [None] * N_SECTION
    value_list = [None] * N_SECTION
    gain_list = [None] * N_SECTION
    for section_index in range(N_SECTION - 1, -1, -1):
        x_rows = inputs[section_index].reshape(MB * N_DP, TOK_DEV, D)
        saved = forward(x_rows, norm_gain[section_index], key_weight[section_index], value_weight[section_index])
        lower_grad, key_back, value_flat, gain_term = backward(upper_grad, *saved, norm_gain[section_index], key_weight[section_index], value_weight[section_index])
        normed = saved[2]
        start = (jnp.zeros((D, KV), jnp.float32), jnp.zeros((D, KV), jnp.float32), jnp.zeros((D,), jnp.float32))
        totals, unused = lax.scan(add_group, start, (regroup(normed), regroup(key_back), regroup(value_flat), regroup(gain_term)))
        key_list[section_index] = totals[0]
        value_list[section_index] = totals[1]
        gain_list[section_index] = totals[2]
        blocks = lower_grad.reshape(MB, TOKENS, D)
        grad_list[section_index] = blocks[plan[section_index]]
        upper_grad = lower_grad
    return (jnp.stack(grad_list), jnp.stack(key_list), jnp.stack(value_list), jnp.stack(gain_list))
```

```python
import functools
import math

import jax
import jax.numpy as jnp
import numpy as np
from jax import lax
from jax.experimental import pallas as pl
from jax.experimental.pallas import tpu as pltpu
from jax.sharding import PartitionSpec as P

HEAD_DIM = 128
EPS = 1e-05
ROPE_BASE = 500000.0
UNITS = 8
DIRECT = (4, 4, 3, 3)
ACROSS = (4, 4, 5, 3)
MESH = pl.DeviceIdType.MESH
F32 = jnp.float32
BF16 = jnp.bfloat16


def dot_nn(a, b):
    return lax.dot_general(a, b, (((1,), (0,)), ((), ())), preferred_element_type=F32)


def dot_nt(a, b):
    return lax.dot_general(a, b, (((1,), (1,)), ((), ())), preferred_element_type=F32)


def dot_tn(a, b):
    return lax.dot_general(a, b, (((0,), (0,)), ((), ())), preferred_element_type=F32)


def rope_tables(length):
    half = HEAD_DIM // 2
    freq = (ROPE_BASE ** (-(np.arange(half, dtype=np.float32) * 2.0 / HEAD_DIM))).astype(np.float32)
    angles = np.arange(length, dtype=np.float32)[:, None] * freq[None, :]
    cos, sin = np.cos(angles), np.sin(angles)
    return (
        np.concatenate([cos, cos], -1).astype(np.float32),
        np.concatenate([-sin, sin], -1).astype(np.float32),
    )


def shares(S):
    if S % 4:
        return False, (UNITS,) * 4, (0,) * 4, (0,) * 4
    return True, DIRECT, ACROSS, tuple(UNITS - d - a for d, a in zip(DIRECT, ACROSS))


def line_slots(S):
    shared, direct, across, near = shares(S)
    before = (across[2], across[3], near[3], 0)
    after = (0, 0, across[0], across[1])
    return max(before[r] + direct[r] + after[r] for r in range(4))


def kernel(S, N, x_ref, cot_ref, gain_ref, wk_ref, wv_ref, cos_ref, sin_ref,
           low_out, gk_out, gv_out, gg_out,
           wall, ns, nall, gall, inv_s, acc, key_s, val_s, qst, prob, ubuf, lowb, gnb,
           kball, gsh, gsall, stage,
           loc, ws, wr, hs, hr, es, er, token, rls, rlr, gsem, nsem, ssem, us, ur, uloc, kbs, kbr, krs, krr):
    B, KH, L = ubuf.shape[0], ubuf.shape[1], ubuf.shape[2]
    CW = ubuf.shape[3]
    w = wall.shape[1]
    KV = KH * HEAD_DIM
    G = CW // HEAD_DIM
    D = x_ref.shape[1]
    C = N // 2
    scale = 1.0 / math.sqrt(HEAD_DIM)
    sec = lax.axis_index("section")
    me = lax.axis_index("dp")
    c = me // 2
    core = me % 2
    partner = c * 2 + (1 - core)
    hp = w // UNITS
    role = sec % 4
    shared, direct, across, near = shares(S)

    def by_role(values):
        out = jnp.int32(values[3])
        for r in range(3):
            out = jnp.where(role == r, jnp.int32(values[r]), out)
        return out

    up = role >= 2
    pair = jnp.where(up, sec - 2, sec + 2) if shared else sec
    first = (direct[2], direct[3], direct[3] + across[3], 0)
    counts = (across[2], across[3], near[3], 0)
    last = (0, 0, direct[0], direct[1])
    after = (0, 0, across[0], across[1])
    lo0, n0 = by_role(first), by_role(counts)
    n1 = by_role(direct)
    lo2, n2 = by_role(last), by_role(after)
    owner0 = jnp.where(role == 2, sec + 1, pair)

    def remote(src, dst, send, recv, peer):
        return pltpu.make_async_remote_copy(
            src_ref=src, dst_ref=dst, send_sem=send, recv_sem=recv,
            device_id=(sec, peer), device_id_type=MESH)

    def wait_all(ref, sem):
        pltpu.make_async_copy(ref, ref, sem).wait()

    ck = pltpu.make_async_copy(wk_ref, wall.at[me, :, pl.ds(0, KV)], loc.at[0])
    cv = pltpu.make_async_copy(wv_ref, wall.at[me, :, pl.ds(KV, KV)], loc.at[1])
    ck.start()
    cv.start()

    barrier = pltpu.get_barrier_semaphore()
    for i in range(1, N):
        pl.semaphore_signal(barrier, inc=1, device_id=(sec, (me + i) % N), device_id_type=MESH)

    @pl.when(sec > 0)
    def _():
        pl.semaphore_signal(barrier, inc=1, device_id=(sec - 1, me), device_id_type=MESH)

    @pl.when(sec < S - 1)
    def _():
        pl.semaphore_signal(barrier, inc=1, device_id=(sec + 1, me), device_id_type=MESH)
    helps = shared
    if helps:
        pl.semaphore_signal(barrier, inc=1, device_id=(pair, me), device_id_type=MESH)
    below = jnp.where(sec > 0, 1, 0)
    above = jnp.where(sec < S - 1, 1, 0)
    pl.semaphore_wait(barrier, N - 1 + below + above + (1 if helps else 0))

    gcopies = []
    for i in range(1, N):
        cp = remote(gain_ref, gall.at[me], gsem.at[0], gsem.at[1], (me + i) % N)
        cp.start()
        gcopies.append(cp)
    gall[me] = gain_ref[...]
    ck.wait()
    cv.wait()

    def piece(shard, p):
        return wall.at[shard, pl.ds(p * hp, hp)]

    def chip_of(way, t):
        return c - 1 - t if way == 0 else c + 1 + t

    def line_copy(way, t, v, ref):
        peer = (c + 1 if way == 0 else c - 1) * 2 + core
        return remote(ref, ref, ws.at[way, t, v], wr.at[way, t, v], peer)

    def held(help_, chip, v, p):
        return stage.at[chip, v] if help_ else piece(chip * 2 + core, p)

    def relay(slot, chip, p, mine):
        ref = piece(chip * 2 + (core if mine else 1 - core), p)
        return remote(ref, ref, rls.at[slot], rlr.at[slot], partner)

    def relayed(slot, chip, mine, sem):
        wait_all(wall.at[chip * 2 + (core if mine else 1 - core)], sem.at[slot])

    def enter(p, v, helper):
        return pltpu.make_async_remote_copy(
            src_ref=piece(me, p), dst_ref=stage.at[c, v], send_sem=es.at[p],
            recv_sem=er.at[v], device_id=(helper, me), device_id_type=MESH)

    def hand(way, t, v, p, owner):
        return pltpu.make_async_remote_copy(
            src_ref=stage.at[chip_of(way, t), v], dst_ref=piece(chip_of(way, t) * 2 + core, p),
            send_sem=hs.at[way, t, v], recv_sem=hr.at[way, t, p],
            device_id=(owner, me), device_id_type=MESH)

    def can_send(way, t):
        return ((c - t >= 0) & (c + 1 < C)) if way == 0 else ((c + t < C) & (c >= 1))

    def can_recv(way, t):
        return (c - 1 - t >= 0) if way == 0 else (c + 1 + t < C)

    def loop(lo, n, f):
        def step(i, carry):
            f(lo + i, i)
            return carry
        lax.fori_loop(0, n, step, 0)

    JOBS = ((lo0, n0, 0, True, owner0), (0, n1, n0, False, sec), (lo2, n2, n0 + n1, True, pair))

    def send_own(job):
        lo, n, base, help_, owner = JOBS[job]

        def one(p, i):
            v = base + i
            if help_:
                enter(p, v, owner).wait_recv()
            for way in range(2):
                @pl.when(can_send(way, 0))
                def _(way=way):
                    line_copy(way, 0, v, held(help_, c, v, p)).start()
        loop(lo, n, one)

    def serve(job, t):
        lo, n, base, help_, owner = JOBS[job]

        def one(p, i):
            v = base + i
            for way in range(2):
                @pl.when(can_recv(way, t))
                def _(way=way):
                    chip = chip_of(way, t)
                    ref = held(help_, chip, v, p)
                    line_copy(way, t, v, ref).wait_recv()
                    if t + 1 < C - 1:
                        @pl.when(can_send(way, t + 1))
                        def _():
                            line_copy(way, t + 1, v, ref).start()
                    if help_:
                        hand(way, t, v, p, owner).start()
                    else:
                        relay(1 + way * (C - 1) + t, chip, p, True).start()
        loop(lo, n, one)

    def handed(t):
        def one(p, i):
            for way in range(2):
                @pl.when(can_recv(way, t))
                def _(way=way):
                    chip = chip_of(way, t)
                    ref = piece(chip * 2 + core, p)
                    remote(ref, ref, hs.at[way, t, 0], hr.at[way, t, p], partner).wait_recv()
                    relay(1 + way * (C - 1) + t, chip, p, True).start()
        loop(n1, UNITS - n1, one)

    def enter_all(act):
        if not shared:
            return
        far = by_role((near[3] + direct[2], direct[3], 0, 0))

        def one(p, i):
            act(enter(p, far + i, pair))
        loop(n1, by_role(across), one)

        @pl.when(role == 3)
        def _():
            def other(p, i):
                act(enter(p, i, sec - 1))
            loop(direct[3] + across[3], near[3], other)

    enter_all(lambda copy: copy.start())

    @pl.when(n0 == 0)
    def _():
        send_own(1)
    remote(wall.at[me], wall.at[me], rls.at[0], rlr.at[0], partner).start()
    send_own(0)

    def cot_copy(k, j):
        return pltpu.make_async_copy(
            cot_ref.at[k, :, pl.ds(j * CW, CW)], ubuf.at[k, j], uloc.at[k, j])

    @pl.when(sec == S - 1)
    def _():
        for k in range(B):
            for j in range(KH):
                cot_copy(k, j).start()

    total = jnp.zeros((B * L, 1), F32)
    for d in range(N):
        xd = x_ref[:, d * w:(d + 1) * w].astype(F32)
        total = total + jnp.sum(xd * xd, axis=-1, keepdims=True)
    inv = lax.rsqrt(total * (1.0 / D) + EPS)
    inv_s[...] = jnp.broadcast_to(inv, inv_s.shape)
    wait_all(gall.at[pl.ds(0, N - 1)], gsem.at[1])
    for d in range(N):
        xd = x_ref[:, d * w:(d + 1) * w].astype(F32)
        ns[d] = (xd * inv * gall[d][0:1, :]).astype(BF16)
        gsh[d] = jnp.zeros(gsh.shape[1:], F32)
    nall[me] = ns[me]
    cos = cos_ref[...]
    sin = sin_ref[...]

    def queries(k, carry):
        rows = pl.ds(pl.multiple_of(k * L, L), L)
        for j in range(KH):
            for g in range(G):
                col = (j * G + g) * HEAD_DIM
                v = ns[col // w, rows, col % w:col % w + HEAD_DIM].astype(F32)
                q = v * cos + pltpu.roll(v, HEAD_DIM // 2, 1) * sin
                qst[k, j, g * L:(g + 1) * L, :] = q.astype(BF16)
        return carry
    lax.fori_loop(0, B, queries, 0)

    def use_step(t):
        for way in range(2):
            @pl.when(can_recv(way, t))
            def _(way=way):
                chip = c - 1 - t if way == 0 else c + 1 + t
                relayed(1 + way * (C - 1) + t, chip, False, rlr)
                acc[...] += dot_nn(ns[chip * 2], wall[chip * 2]) + dot_nn(
                    ns[chip * 2 + 1], wall[chip * 2 + 1])

    def send_rows():
        for i in range(1, N):
            peer = (me + i) % N
            remote(ns.at[peer], nall.at[me], nsem.at[0], nsem.at[1], peer).start()

    for t in range(C - 1):
        serve(0, t)
        if t == 0:
            @pl.when(n0 > 0)
            def _():
                send_own(1)
    relayed(0, c, False, rlr)
    acc[...] = dot_nn(ns[c * 2], wall[c * 2]) + dot_nn(ns[c * 2 + 1], wall[c * 2 + 1])
    for t in range(C - 1):
        serve(1, t)
        if t == 0:
            send_own(2)
        if t > 0:
            handed(t - 1)
        if t > 1:
            use_step(t - 2)
    handed(C - 2)
    if C > 2:
        use_step(C - 3)
    use_step(C - 2)

    @pl.when(n2 == 0)
    def _():
        send_rows()

    row_pos = lax.broadcasted_iota(jnp.int32, (L, L), 0)
    col_pos = lax.broadcasted_iota(jnp.int32, (L, L), 1)
    causal = (row_pos >= col_pos)[None]

    def attend(k, carry):
        rows = pl.ds(pl.multiple_of(k * L, L), L)
        for j in range(KH):
            kp = acc[rows, j * HEAD_DIM:(j + 1) * HEAD_DIM]
            key = (kp * cos + pltpu.roll(kp, HEAD_DIM // 2, 1) * sin).astype(BF16)
            key_s[k, j] = key
            val_s[k, j] = acc[rows, KV + j * HEAD_DIM:KV + (j + 1) * HEAD_DIM].astype(BF16)
            sc = dot_nt(qst[k, j], key) * scale
            raised = jnp.where(causal, jnp.exp(sc.reshape(G, L, L)), 0.0)
            pr = raised / jnp.sum(raised, axis=-1, keepdims=True)
            prob[k, j] = pr.reshape(G * L, L)
        return carry
    lax.fori_loop(0, B, attend, 0)

    def usend(k, j):
        return pltpu.make_async_remote_copy(
            src_ref=lowb.at[k, j], dst_ref=ubuf.at[k, j], send_sem=us.at[k, j],
            recv_sem=ur.at[k, j], device_id=(lax.max(sec - 1, 0), me), device_id_type=MESH)

    def kbcopy(k, j, i):
        peer = ((c + i) % C) * 2 + core
        ref = kball.at[me, k, j]
        return remote(ref, ref, kbs.at[k, i], kbr.at[k, i], peer)

    def kbpartner(k, j):
        ref = kball.at[me, k, j]
        return remote(ref, ref, kbs.at[k, 0], kbr.at[k, 0], partner)

    def kbrelay(k, i, mine):
        chip = (c - i + C) % C
        ref = kball.at[chip * 2 + (core if mine else 1 - core), k]
        return remote(ref, ref, krs.at[k, i], krr.at[k, i], partner)

    def sent(k):
        @pl.when(sec > 0)
        def _():
            for j in range(KH):
                usend(k, j).wait_send()

    def turn(k, carry):
        rows = pl.ds(pl.multiple_of(k * L, L), L)
        keys, values = [], []
        for j in range(KH):
            @pl.when(sec == S - 1)
            def _(j=j):
                cot_copy(k, j).wait()

            @pl.when(sec < S - 1)
            def _(j=j):
                usend(k, j).wait_recv()
            u = ubuf[k, j]
            us_ = jnp.concatenate(
                [u[:, g * HEAD_DIM:(g + 1) * HEAD_DIM] for g in range(G)], axis=0)
            key, q, pr = key_s[k, j], qst[k, j], prob[k, j]
            gp = dot_nt(us_, val_s[k, j])
            gv = dot_tn(pr.astype(BF16), us_).astype(BF16)
            rd = jnp.sum(pr * gp, axis=-1, keepdims=True)
            gs = (pr * (gp - rd) * scale).astype(BF16)
            gk = dot_tn(gs, q)
            gk = (gk * cos - pltpu.roll(gk, HEAD_DIM // 2, 1) * sin).astype(BF16)
            keys.append(gk)
            values.append(gv)
            kball[me, k, j] = jnp.concatenate([gk, gv], axis=1)
            gq = dot_nn(gs, key)
            for g in range(G):
                v = gq[g * L:(g + 1) * L]
                col = (j * G + g) * HEAD_DIM
                gnb[col // w, :, col % w:col % w + HEAD_DIM] = (
                    v * cos - pltpu.roll(v, HEAD_DIM // 2, 1) * sin)
            kbpartner(k, j).start()
            for i in range(1, C):
                kbcopy(k, j, i).start()
        @pl.when((sec == S - 1) & (k > 0))
        def _():
            sent(k - 1)
            pl.semaphore_signal(token, inc=1, device_id=(sec, partner), device_id_type=MESH)
        kbv = jnp.concatenate(keys + values, axis=1)
        part_inv = inv_s[rows, 0:1]
        proj = jnp.zeros((L, 1), F32)
        for d in range(N):
            gn = gnb[d] + dot_nt(kbv, wall[d])
            gnb[d] = gn
            gt = gn * x_ref[rows, d * w:(d + 1) * w].astype(F32) * part_inv
            proj = proj + jnp.sum(gt * gall[d][0:1, :], axis=-1, keepdims=True)
            gsh[d] += jnp.sum(gt.reshape(L // 8, 8, w), axis=0)
        proj = proj * (1.0 / D) * part_inv * part_inv
        @pl.when((sec == S - 1) & ((k > 0) | (core > 0)))
        def _():
            pl.semaphore_wait(token, 1)
        for j in range(KH):
            for e in range(N // KH):
                d = j * (N // KH) + e
                u = ubuf[k, j, :, e * w:(e + 1) * w].astype(F32)
                xd = x_ref[rows, d * w:(d + 1) * w].astype(F32)
                low = (u + part_inv * gall[d][0:1, :] * gnb[d] - xd * proj).astype(BF16)
                lowb[k, j, :, e * w:(e + 1) * w] = low
                low_out[rows, d * w:(d + 1) * w] = low

            @pl.when(sec > 0)
            def _(j=j):
                usend(k, j).start()
        return carry
    lax.fori_loop(0, B, turn, 0)

    for t in range(C - 1):
        serve(2, t)

    @pl.when(n2 > 0)
    def _():
        send_rows()

    @pl.when((sec == S - 1) & (core == 0))
    def _():
        sent(B - 1)
        pl.semaphore_signal(token, inc=1, device_id=(sec, partner), device_id_type=MESH)

    gsall[me] = gsh[me]
    for i in range(1, N):
        peer = (me + i) % N
        remote(gsh.at[peer], gsall.at[me], ssem.at[0], ssem.at[1], peer).start()
    for k in range(B):
        for i in range(1, C):
            chip = (c - i + C) % C
            wait_all(kball.at[chip * 2 + core, k], kbr.at[k, i])
            kbrelay(k, i, True).start()
    wait_all(nall.at[pl.ds(0, N - 1)], nsem.at[1])
    for k in range(B):
        wait_all(kball.at[partner, k], kbr.at[k, 0])
        for i in range(1, C):
            kbrelay(k, i, False).wait_recv()
    rows_all = nall[...].reshape(N * B * L, w)
    for j in range(KH):
        back = jnp.concatenate(
            [kball[g, k, j] for g in range(N) for k in range(B)], axis=0)
        dw = dot_tn(rows_all, back)
        gk_out[:, j * HEAD_DIM:(j + 1) * HEAD_DIM] = dw[:, :HEAD_DIM]
        gv_out[:, j * HEAD_DIM:(j + 1) * HEAD_DIM] = dw[:, HEAD_DIM:]
    wait_all(gsall.at[pl.ds(0, N - 1)], ssem.at[1])
    gg = gsall[0]
    for d in range(1, N):
        gg = gg + gsall[d]
    gg_out[...] = jnp.broadcast_to(jnp.sum(gg, axis=0, keepdims=True), gg_out.shape)

    wait_all(gall.at[pl.ds(0, N - 1)], gsem.at[0])
    wait_all(nall.at[pl.ds(0, N - 1)], nsem.at[0])
    wait_all(gsall.at[pl.ds(0, N - 1)], ssem.at[0])
    relayed(0, c, True, rls)
    enter_all(lambda copy: copy.wait_send())
    for t in range(C - 1):
        for job in range(3):
            lo, n, base, help_, owner = JOBS[job]

            def done(p, i, t=t, base=base, help_=help_, owner=owner):
                v = base + i
                for way in range(2):
                    @pl.when(can_send(way, t))
                    def _(way=way):
                        line_copy(way, t, v, held(help_, c, v, p)).wait_send()
                    if help_:
                        @pl.when(can_recv(way, t))
                        def _(way=way):
                            hand(way, t, v, p, owner).wait_send()
            loop(lo, n, done)
        for way in range(2):
            @pl.when(can_recv(way, t))
            def _(way=way, t=t):
                relayed(1 + way * (C - 1) + t, chip_of(way, t), True, rls)
    for k in range(B):
        for i in range(C):
            wait_all(kball.at[me, k], kbs.at[k, i])
            if i:
                kbrelay(k, i, True).wait_send()

    @pl.when(sec < S - 1)
    def _():
        for k in range(B):
            sent(k)

    @pl.when((sec == S - 1) & (core == 1))
    def _():
        sent(B - 1)


def body(S, N, inputs, cotangent, norm_gain, key_weight, value_weight, plan):
    B, L, D = inputs.shape[1:]
    w, KV = key_weight.shape[1:]
    KH = KV // HEAD_DIM
    CW = D // KH
    G = CW // HEAD_DIM
    C = N // 2
    slots = line_slots(S)
    cos, sin = rope_tables(L)
    gain8 = jnp.broadcast_to(norm_gain.astype(F32), (8, w))
    vmem = pl.BlockSpec(memory_space=pltpu.VMEM)
    hbm = pl.BlockSpec(memory_space=pl.ANY)
    dma = pltpu.SemaphoreType.DMA
    low, gk, gv, gg = pl.pallas_call(
        functools.partial(kernel, S, N),
        out_shape=(
            jax.ShapeDtypeStruct((B * L, D), BF16),
            jax.ShapeDtypeStruct((w, KV), F32),
            jax.ShapeDtypeStruct((w, KV), F32),
            jax.ShapeDtypeStruct((8, w), F32),
        ),
        in_specs=[vmem, hbm, vmem, hbm, hbm, vmem, vmem],
        out_specs=(vmem,) * 4,
        scratch_shapes=[
            pltpu.VMEM((N, w, 2 * KV), BF16),
            pltpu.VMEM((N, B * L, w), BF16),
            pltpu.VMEM((N, B * L, w), BF16),
            pltpu.VMEM((N, 8, w), F32),
            pltpu.VMEM((B * L, 128), F32),
            pltpu.VMEM((B * L, 2 * KV), F32),
            pltpu.VMEM((B, KH, L, HEAD_DIM), BF16),
            pltpu.VMEM((B, KH, L, HEAD_DIM), BF16),
            pltpu.VMEM((B, KH, G * L, HEAD_DIM), BF16),
            pltpu.VMEM((B, KH, G * L, L), F32),
            pltpu.VMEM((B, KH, L, CW), BF16),
            pltpu.VMEM((B, KH, L, CW), BF16),
            pltpu.VMEM((N, L, w), F32),
            pltpu.VMEM((N, B, KH, L, 2 * HEAD_DIM), BF16),
            pltpu.VMEM((N, 8, w), F32),
            pltpu.VMEM((N, 8, w), F32),
            pltpu.VMEM((C, slots, w // UNITS, 2 * KV), BF16),
            dma((2,)),
            dma((2, C - 1, slots)),
            dma((2, C - 1, slots)),
            dma((2, C - 1, slots)),
            dma((2, C - 1, UNITS)),
            dma((UNITS,)),
            dma((slots,)),
            pltpu.SemaphoreType.REGULAR,
            dma((2 * C - 1,)),
            dma((2 * C - 1,)),
            dma((2,)),
            dma((2,)),
            dma((2,)),
            dma((B, KH)),
            dma((B, KH)),
            dma((B, KH)),
            dma((B, C)),
            dma((B, C)),
            dma((B, C)),
            dma((B, C)),
        ],
        compiler_params=pltpu.CompilerParams(
            collective_id=0, has_side_effects=True, vmem_limit_bytes=56 * 1024 * 1024),
    )(inputs[0].reshape(B * L, D), cotangent, gain8, key_weight[0], value_weight[0],
      jnp.asarray(cos), jnp.asarray(sin))
    low = low.reshape(B, L, D)
    selector = plan[0][:, None] == jnp.arange(B, dtype=jnp.int32)[None, :]
    ordered = jnp.sum(
        jnp.where(selector[:, :, None, None], low[None], jnp.zeros((), BF16)), axis=1)
    return ordered[None], gk[None], gv[None], gg[0:1]


def solution(mesh):
    in_specs = (
        P("section", None, "dp", None),
        P(None, "dp", None),
        P("section", "dp"),
        P("section", "dp", None),
        P("section", "dp", None),
        P("section", None),
    )
    out_specs = (
        P("section", None, "dp", None),
        P("section", "dp", None),
        P("section", "dp", None),
        P("section", "dp"),
    )
    run = functools.partial(body, mesh.shape["section"], mesh.shape["dp"])
    return jax.shard_map(run, mesh=mesh, in_specs=in_specs, out_specs=out_specs, check_vma=False)
```

```python
import functools
import math

import jax
import jax.numpy as jnp
import numpy as np
from jax import lax
from jax.experimental import pallas as pl
from jax.experimental.pallas import tpu as pltpu
from jax.sharding import PartitionSpec as P

HEAD_DIM = 128
EPS = 1e-05
ROPE_BASE = 500000.0
DIRECT = (8, 9, 7, 6)
ACROSS = (5, 7, 9, 5)
MESH = pl.DeviceIdType.MESH
F32 = jnp.float32
BF16 = jnp.bfloat16


def dot_nn(a, b):
    return lax.dot_general(a, b, (((1,), (0,)), ((), ())), preferred_element_type=F32)


def dot_nt(a, b):
    return lax.dot_general(a, b, (((1,), (1,)), ((), ())), preferred_element_type=F32)


def dot_tn(a, b):
    return lax.dot_general(a, b, (((0,), (0,)), ((), ())), preferred_element_type=F32)


def rope_tables(length):
    half = HEAD_DIM // 2
    freq = (ROPE_BASE ** (-(np.arange(half, dtype=np.float32) * 2.0 / HEAD_DIM))).astype(np.float32)
    angles = np.arange(length, dtype=np.float32)[:, None] * freq[None, :]
    cos, sin = np.cos(angles), np.sin(angles)
    return (
        np.concatenate([cos, cos], -1).astype(np.float32),
        np.concatenate([-sin, sin], -1).astype(np.float32),
    )


def shares(S, w):
    units = 16 if w % 256 == 0 else 8
    if S % 4:
        return units, False, (units,) * 4, (0,) * 4, (0,) * 4
    direct = tuple(d * units // 16 for d in DIRECT)
    across = tuple(a * units // 16 if r in (0, 3) else units - direct[r] for r, a in enumerate(ACROSS))
    return units, True, direct, across, tuple(units - d - a for d, a in zip(direct, across))


def line_slots(S, w):
    units, shared, direct, across, near = shares(S, w)
    before = (across[2], across[3], near[3], 0)
    after = (0, 0, across[0], across[1] + near[0])
    return max(before[r] + direct[r] + after[r] for r in range(4))


def kernel(S, N, x_ref, cot_ref, gain_ref, wk_ref, wv_ref, cos_ref, sin_ref,
           low_out, gk_out, gv_out, gg_out,
           wall, ns, nall, gall, inv_s, acc, key_s, val_s, qst, prob, ubuf, lowb, gnb,
           kball, gsh, gsall, stage,
           loc, ws, wr, hs, hr, es, er, token, release, rls, rlr, gsem, nsem, ssem, us, ur, uloc, kbs, kbr, krs, krr, kfs):
    B, KH, L = ubuf.shape[0], ubuf.shape[1], ubuf.shape[2]
    CW = ubuf.shape[3]
    w = wall.shape[1]
    KV = KH * HEAD_DIM
    G = CW // HEAD_DIM
    D = x_ref.shape[1]
    C = N // 2
    scale = 1.0 / math.sqrt(HEAD_DIM)
    sec = lax.axis_index("section")
    me = lax.axis_index("dp")
    c = me // 2
    core = me % 2
    partner = c * 2 + (1 - core)
    role = sec % 4
    UNITS, shared, direct, across, near = shares(S, w)
    hp = w // UNITS

    def by_role(values):
        out = jnp.int32(values[3])
        for r in range(3):
            out = jnp.where(role == r, jnp.int32(values[r]), out)
        return out

    up = role >= 2
    pair = jnp.where(up, sec - 2, sec + 2) if shared else sec
    first = (direct[2], direct[3], direct[3] + across[3], 0)
    counts = (across[2], across[3], near[3], 0)
    last = (0, 0, direct[0], direct[1])
    after = (0, 0, across[0], across[1])
    lo0, n0 = by_role(first), by_role(counts)
    n1 = by_role(direct)
    lo2, n2 = by_role(last), by_role(after)
    owner0 = jnp.where(role == 2, sec + 1, pair)
    n3 = by_role((0, 0, 0, near[0]))

    def remote(src, dst, send, recv, peer):
        return pltpu.make_async_remote_copy(
            src_ref=src, dst_ref=dst, send_sem=send, recv_sem=recv,
            device_id=(sec, peer), device_id_type=MESH)

    def wait_all(ref, sem):
        pltpu.make_async_copy(ref, ref, sem).wait()

    ck = pltpu.make_async_copy(wk_ref, wall.at[me, :, pl.ds(0, KV)], loc.at[0])
    cv = pltpu.make_async_copy(wv_ref, wall.at[me, :, pl.ds(KV, KV)], loc.at[1])
    ck.start()
    cv.start()

    barrier = pltpu.get_barrier_semaphore()
    for i in range(1, N):
        pl.semaphore_signal(barrier, inc=1, device_id=(sec, (me + i) % N), device_id_type=MESH)

    @pl.when(sec > 0)
    def _():
        pl.semaphore_signal(barrier, inc=1, device_id=(sec - 1, me), device_id_type=MESH)

    @pl.when(sec < S - 1)
    def _():
        pl.semaphore_signal(barrier, inc=1, device_id=(sec + 1, me), device_id_type=MESH)
    if shared:
        first_sec = sec - role
        for step in range(1, 4):
            for i in range(C):
                pl.semaphore_signal(
                    barrier, inc=1, device_id=(first_sec + (role + step) % 4, i * 2 + core),
                    device_id_type=MESH)
    below = jnp.where(sec > 0, 1, 0)
    above = jnp.where(sec < S - 1, 1, 0)
    pl.semaphore_wait(barrier, N - 1 + below + above + (3 * C if shared else 0))

    gcopies = []
    for i in range(1, N):
        cp = remote(gain_ref, gall.at[me], gsem.at[0], gsem.at[1], (me + i) % N)
        cp.start()
        gcopies.append(cp)
    gall[me] = gain_ref[...]
    ck.wait()
    cv.wait()

    def piece(shard, p):
        return wall.at[shard, pl.ds(p * hp, hp)]

    def chip_of(way, t):
        return c - 1 - t if way == 0 else c + 1 + t

    def line_copy(way, t, v, ref):
        peer = (c + 1 if way == 0 else c - 1) * 2 + core
        return remote(ref, ref, ws.at[way, t, v], wr.at[way, t, v], peer)

    def relay(slot, chip, p, mine):
        ref = piece(chip * 2 + (core if mine else 1 - core), p)
        return remote(ref, ref, rls.at[slot], rlr.at[slot], partner)

    def relayed(slot, chip, mine, sem):
        wait_all(wall.at[chip * 2 + (core if mine else 1 - core)], sem.at[slot])

    def enter(p, v, helper):
        return pltpu.make_async_remote_copy(
            src_ref=piece(me, p), dst_ref=stage.at[c, v], send_sem=es.at[p],
            recv_sem=er.at[v], device_id=(helper, me), device_id_type=MESH)

    def deliver(way, chip, kind, t, v, p, owner):
        peer = (chip + t + 1 if way == 0 else chip - t - 1) * 2 + core
        return pltpu.make_async_remote_copy(
            src_ref=stage.at[chip, v], dst_ref=piece(chip * 2 + core, p),
            send_sem=hs.at[kind, way, t, v], recv_sem=hr.at[way, t, p],
            device_id=(owner, peer), device_id_type=MESH)

    def relay_on(way, chip, t, v):
        peer = (chip + t + 1 if way == 0 else chip - t - 1) * 2 + core
        ref = stage.at[chip, v]
        return remote(ref, ref, ws.at[way, t, v], wr.at[way, t, v], peer)

    def can_send(way, t):
        return ((c - t >= 0) & (c + 1 < C)) if way == 0 else ((c + t < C) & (c >= 1))

    def can_recv(way, t):
        return (c - 1 - t >= 0) if way == 0 else (c + 1 + t < C)

    def loop(lo, n, f):
        def step(i, carry):
            f(lo + i, i)
            return carry
        lax.fori_loop(0, n, step, 0)

    JOBS = (
        (lo0, n0, 0, owner0),
        (lo2, n2, n0 + n1, pair),
        (direct[0] + across[0], n3, n0 + n1 + n2, sec - 3),
    )

    def left_over(way):
        return C - 1 - c if way == 0 else c

    def spread_far(way, chip, a, v, act):
        @pl.when(left_over(way) >= 3)
        def _():
            act(relay_on(way, chip, a + 1, v))

    def spread_near(way, chip, a, v, p, owner, act):
        left = left_over(way)

        @pl.when(left == 2)
        def _():
            act(deliver(way, chip, 0, a + 1, v, p, owner))

        @pl.when(left >= 1)
        def _():
            act(deliver(way, chip, 0, a, v, p, owner))

    def spread(way, chip, a, v, p, owner, act):
        spread_far(way, chip, a, v, act)
        spread_near(way, chip, a, v, p, owner, act)

    far_end = (left_over(0) >= 3) | (left_over(1) >= 3)

    def start(copy):
        copy.start()

    def sent_out(copy):
        copy.wait_send()

    def own_sends(act):
        def one(p, i):
            for way in range(2):
                @pl.when(can_send(way, 0))
                def _(way=way):
                    act(line_copy(way, 0, n0 + i, piece(c * 2 + core, p)))
        loop(0, n1, one)

    def help_far(job, act, arrive):
        lo, n, base, owner = JOBS[job]

        def one(p, i):
            @pl.when(far_end)
            def _():
                if arrive:
                    enter(p, base + i, owner).wait_recv()
                for way in range(2):
                    spread_far(way, c, 0, base + i, act)
        loop(lo, n, one)

    def help_near(job, act, arrive):
        lo, n, base, owner = JOBS[job]

        def one(p, i):
            if arrive:
                @pl.when(jnp.logical_not(far_end))
                def _():
                    enter(p, base + i, owner).wait_recv()
            for way in range(2):
                spread_near(way, c, 0, base + i, p, owner, act)
        loop(lo, n, one)

    def help_on(job, act, arrive):
        lo, n, base, owner = JOBS[job]
        for t in range(1, C - 1, 2):
            def one(p, i, t=t):
                v = base + i
                for way in range(2):
                    @pl.when(can_recv(way, t) & (left_over(way) >= 1))
                    def _(way=way):
                        chip = chip_of(way, t)
                        if arrive:
                            relay_on(way, chip, t, v).wait_recv()
                        spread(way, chip, t + 1, v, p, owner, act)
                        act(deliver(way, chip, 1, t, v, p, owner))
            loop(lo, n, one)

    def serve(t):
        def one(p, i):
            v = n0 + i
            for way in range(2):
                @pl.when(can_recv(way, t))
                def _(way=way):
                    chip = chip_of(way, t)
                    ref = piece(chip * 2 + core, p)
                    line_copy(way, t, v, ref).wait_recv()
                    if t + 1 < C - 1:
                        @pl.when(can_send(way, t + 1))
                        def _():
                            line_copy(way, t + 1, v, ref).start()
                    relay(1 + way * (C - 1) + t, chip, p, True).start()
        loop(0, n1, one)

    def handed(t):
        def one(p, i):
            for way in range(2):
                @pl.when(can_recv(way, t))
                def _(way=way):
                    chip = chip_of(way, t)
                    ref = piece(chip * 2 + core, p)
                    remote(ref, ref, hs.at[way, t, 0], hr.at[way, t, p], partner).wait_recv()
                    relay(1 + way * (C - 1) + t, chip, p, True).start()
        loop(n1, UNITS - n1, one)

    def enter_all(act):
        if not shared:
            return
        far = by_role((near[3] + direct[2], direct[3], 0, 0))

        def one(p, i):
            act(enter(p, far + i, pair))
        loop(n1, by_role(across), one)
        for r, base, step in ((3, 0, -1), (0, direct[3] + across[1], 3)):
            @pl.when(role == r)
            def _(r=r, base=base, step=step):
                def other(p, i):
                    act(enter(p, base + i, sec + step))
                loop(direct[r] + across[r], near[r], other)

    enter_all(start)

    @pl.when(n0 == 0)
    def _():
        own_sends(start)
    remote(wall.at[me], wall.at[me], rls.at[0], rlr.at[0], partner).start()
    help_far(0, start, True)
    help_near(0, start, True)

    def cot_copy(k, j):
        return pltpu.make_async_copy(
            cot_ref.at[k, :, pl.ds(j * CW, CW)], ubuf.at[k, j], uloc.at[k, j])

    @pl.when(sec == S - 1)
    def _():
        for k in range(B):
            for j in range(KH):
                cot_copy(k, j).start()

    total = jnp.zeros((B * L, 1), F32)
    for d in range(N):
        xd = x_ref[:, d * w:(d + 1) * w].astype(F32)
        total = total + jnp.sum(xd * xd, axis=-1, keepdims=True)
    inv = lax.rsqrt(total * (1.0 / D) + EPS)
    inv_s[...] = jnp.broadcast_to(inv, inv_s.shape)
    wait_all(gall.at[pl.ds(0, N - 1)], gsem.at[1])
    for d in range(N):
        xd = x_ref[:, d * w:(d + 1) * w].astype(F32)
        ns[d] = (xd * inv * gall[d][0:1, :]).astype(BF16)
        gsh[d] = jnp.zeros(gsh.shape[1:], F32)
    nall[me] = ns[me]
    cos = cos_ref[...]
    sin = sin_ref[...]

    def queries(k, carry):
        rows = pl.ds(pl.multiple_of(k * L, L), L)
        for j in range(KH):
            for g in range(G):
                col = (j * G + g) * HEAD_DIM
                v = ns[col // w, rows, col % w:col % w + HEAD_DIM].astype(F32)
                q = v * cos + pltpu.roll(v, HEAD_DIM // 2, 1) * sin
                qst[k, j, g * L:(g + 1) * L, :] = q.astype(BF16)
        return carry
    lax.fori_loop(0, B, queries, 0)

    def use_step(t):
        for way in range(2):
            @pl.when(can_recv(way, t))
            def _(way=way):
                chip = c - 1 - t if way == 0 else c + 1 + t
                relayed(1 + way * (C - 1) + t, chip, False, rlr)
                acc[...] += dot_nn(ns[chip * 2], wall[chip * 2]) + dot_nn(
                    ns[chip * 2 + 1], wall[chip * 2 + 1])

    help_on(0, start, True)

    @pl.when(n0 > 0)
    def _():
        own_sends(start)
    relayed(0, c, False, rlr)
    acc[...] = dot_nn(ns[c * 2], wall[c * 2]) + dot_nn(ns[c * 2 + 1], wall[c * 2 + 1])
    for t in range(C - 1):
        serve(t)
        if 0 < t < C - 2:
            handed(t - 1)

    for job in (1, 2):
        help_far(job, start, True)
    for job in (1, 2):
        help_near(job, start, True)

    def send_rows():
        for i in range(1, N):
            peer = (me + i) % N
            remote(ns.at[peer], nall.at[me], nsem.at[0], nsem.at[1], peer).start()

    @pl.when((role < 2) if shared else (role >= 0))
    def _():
        send_rows()
    if C > 2:
        handed(C - 3)
    for t in range(C - 2):
        use_step(t)
    handed(C - 2)
    use_step(C - 2)

    row_pos = lax.broadcasted_iota(jnp.int32, (L, L), 0)
    col_pos = lax.broadcasted_iota(jnp.int32, (L, L), 1)
    causal = (row_pos >= col_pos)[None]

    def attend(k, carry):
        rows = pl.ds(pl.multiple_of(k * L, L), L)
        for j in range(KH):
            kp = acc[rows, j * HEAD_DIM:(j + 1) * HEAD_DIM]
            key = (kp * cos + pltpu.roll(kp, HEAD_DIM // 2, 1) * sin).astype(BF16)
            key_s[k, j] = key
            val_s[k, j] = acc[rows, KV + j * HEAD_DIM:KV + (j + 1) * HEAD_DIM].astype(BF16)
            sc = dot_nt(qst[k, j], key) * scale
            raised = jnp.where(causal, jnp.exp(sc.reshape(G, L, L)), 0.0)
            pr = raised / jnp.sum(raised, axis=-1, keepdims=True)
            prob[k, j] = pr.reshape(G * L, L)
        return carry
    lax.fori_loop(0, B, attend, 0)

    def usend(k, j):
        return pltpu.make_async_remote_copy(
            src_ref=lowb.at[k, j], dst_ref=ubuf.at[k, j], send_sem=us.at[k, j],
            recv_sem=ur.at[k, j], device_id=(lax.max(sec - 1, 0), me), device_id_type=MESH)

    def kbcopy(k, j, i):
        peer = ((c + i) % C) * 2 + core
        ref = kball.at[me, k, j]
        return remote(ref, ref, kbs.at[k, i], kbr.at[k, i], peer)

    def kbpartner(k, j):
        ref = kball.at[me, k, j]
        return remote(ref, ref, kbs.at[k, 0], kbr.at[k, 0], partner)

    def kbsends(k, j, i):
        right = (i == 1) & (c + 1 < C)
        left = (i == C - 1) & (c >= 1)
        return (sec == 0) | right | left

    def kbshare(k, j):
        kbpartner(k, j).start()
        for i in range(1, C):
            @pl.when(kbsends(k, j, i))
            def _(i=i):
                kbcopy(k, j, i).start()

    def from_chip(way, t):
        return t + 1 if way == 0 else C - 1 - t

    def kbpass(k, way, t):
        ref = kball.at[chip_of(way, t) * 2 + core, k]
        peer = (c + 1 if way == 0 else c - 1) * 2 + core
        return remote(ref, ref, kfs.at[k, way, t], kbr.at[k, from_chip(way, t + 1)], peer)

    def kbrelay(k, i, mine):
        chip = (c - i + C) % C
        ref = kball.at[chip * 2 + (core if mine else 1 - core), k]
        return remote(ref, ref, krs.at[k, i], krr.at[k, i], partner)

    def sent(k):
        @pl.when(sec > 0)
        def _():
            for j in range(KH):
                usend(k, j).wait_send()

    def turn(k, carry):
        rows = pl.ds(pl.multiple_of(k * L, L), L)
        keys, values = [], []

        @pl.when((k == B - 1) & (role >= 2))
        def _():
            for job in (1, 2):
                help_on(job, start, True)
        for j in range(KH):
            @pl.when(sec == S - 1)
            def _(j=j):
                cot_copy(k, j).wait()

            @pl.when(sec < S - 1)
            def _(j=j):
                usend(k, j).wait_recv()
            u = ubuf[k, j]
            us_ = jnp.concatenate(
                [u[:, g * HEAD_DIM:(g + 1) * HEAD_DIM] for g in range(G)], axis=0)
            key, q, pr = key_s[k, j], qst[k, j], prob[k, j]
            gp = dot_nt(us_, val_s[k, j])
            gv = dot_tn(pr.astype(BF16), us_).astype(BF16)
            rd = jnp.sum(pr * gp, axis=-1, keepdims=True)
            gs = (pr * (gp - rd) * scale).astype(BF16)
            gk = dot_tn(gs, q)
            gk = (gk * cos - pltpu.roll(gk, HEAD_DIM // 2, 1) * sin).astype(BF16)
            keys.append(gk)
            values.append(gv)
            kball[me, k, j] = jnp.concatenate([gk, gv], axis=1)
            gq = dot_nn(gs, key)
            for g in range(G):
                v = gq[g * L:(g + 1) * L]
                col = (j * G + g) * HEAD_DIM
                gnb[col // w, :, col % w:col % w + HEAD_DIM] = (
                    v * cos - pltpu.roll(v, HEAD_DIM // 2, 1) * sin)
            @pl.when(sec == 0)
            def _(j=j):
                kbshare(k, j)
        @pl.when((sec == S - 1) & (k > 0))
        def _():
            sent(k - 1)
            pl.semaphore_signal(token, inc=1, device_id=(sec, partner), device_id_type=MESH)
        kbv = jnp.concatenate(keys + values, axis=1)
        part_inv = inv_s[rows, 0:1]
        proj = jnp.zeros((L, 1), F32)
        for d in range(N):
            gn = gnb[d] + dot_nt(kbv, wall[d])
            gnb[d] = gn
            gt = gn * x_ref[rows, d * w:(d + 1) * w].astype(F32) * part_inv
            proj = proj + jnp.sum(gt * gall[d][0:1, :], axis=-1, keepdims=True)
            gsh[d] += jnp.sum(gt.reshape(L // 8, 8, w), axis=0)
        proj = proj * (1.0 / D) * part_inv * part_inv
        @pl.when((sec == S - 1) & ((k > 0) | (core > 0)))
        def _():
            pl.semaphore_wait(token, 1)
        for j in range(KH):
            for e in range(N // KH):
                d = j * (N // KH) + e
                u = ubuf[k, j, :, e * w:(e + 1) * w].astype(F32)
                xd = x_ref[rows, d * w:(d + 1) * w].astype(F32)
                low = (u + part_inv * gall[d][0:1, :] * gnb[d] - xd * proj).astype(BF16)
                lowb[k, j, :, e * w:(e + 1) * w] = low
                low_out[rows, d * w:(d + 1) * w] = low

            @pl.when(sec > 0)
            def _(j=j):
                usend(k, j).start()
        return carry
    lax.fori_loop(0, B, turn, 0)

    for job in range(3):
        help_far(job, sent_out, False)
        help_near(job, sent_out, False)
        help_on(job, sent_out, False)
    if shared:
        @pl.when(role >= 2)
        def _():
            half = C // 2

            @pl.when((c >= 1) & (c < half))
            def _():
                pl.semaphore_signal(release, inc=1, device_id=(sec, me - 2), device_id_type=MESH)

            @pl.when((c >= half) & (c < C - 1))
            def _():
                pl.semaphore_signal(release, inc=1, device_id=(sec, me + 2), device_id_type=MESH)

            @pl.when((c < half - 1) | (c > half))
            def _():
                pl.semaphore_wait(release, 1)
            send_rows()

    @pl.when(sec > 0)
    def _():
        for k in range(B):
            for j in range(KH):
                kbshare(k, j)

    @pl.when((sec == S - 1) & (core == 0))
    def _():
        sent(B - 1)
        pl.semaphore_signal(token, inc=1, device_id=(sec, partner), device_id_type=MESH)

    gsall[me] = gsh[me]
    for i in range(1, N):
        peer = (me + i) % N
        remote(gsh.at[peer], gsall.at[me], ssem.at[0], ssem.at[1], peer).start()
    for k in range(B):
        for t in range(C - 1):
            for way in range(2):
                @pl.when(can_recv(way, t))
                def _(k=k, t=t, way=way):
                    i = from_chip(way, t)
                    wait_all(kball.at[chip_of(way, t) * 2 + core, k], kbr.at[k, i])
                    if t + 1 < C - 1:
                        @pl.when((sec > 0) & can_send(way, t + 1))
                        def _():
                            kbpass(k, way, t).start()
                    kbrelay(k, i, True).start()
    wait_all(nall.at[pl.ds(0, N - 1)], nsem.at[1])
    for k in range(B):
        wait_all(kball.at[partner, k], kbr.at[k, 0])
        for i in range(1, C):
            kbrelay(k, i, False).wait_recv()
    rows_all = nall[...].reshape(N * B * L, w)
    for j in range(KH):
        back = jnp.concatenate(
            [kball[g, k, j] for g in range(N) for k in range(B)], axis=0)
        dw = dot_tn(rows_all, back)
        gk_out[:, j * HEAD_DIM:(j + 1) * HEAD_DIM] = dw[:, :HEAD_DIM]
        gv_out[:, j * HEAD_DIM:(j + 1) * HEAD_DIM] = dw[:, HEAD_DIM:]
    wait_all(gsall.at[pl.ds(0, N - 1)], ssem.at[1])
    gg = gsall[0]
    for d in range(1, N):
        gg = gg + gsall[d]
    gg_out[...] = jnp.broadcast_to(jnp.sum(gg, axis=0, keepdims=True), gg_out.shape)

    wait_all(gall.at[pl.ds(0, N - 1)], gsem.at[0])
    wait_all(nall.at[pl.ds(0, N - 1)], nsem.at[0])
    wait_all(gsall.at[pl.ds(0, N - 1)], ssem.at[0])
    relayed(0, c, True, rls)
    enter_all(sent_out)
    own_sends(sent_out)
    for t in range(C - 1):
        def passed(p, i, t=t):
            for way in range(2):
                @pl.when(can_recv(way, t) & can_send(way, t + 1))
                def _(way=way):
                    ref = piece(chip_of(way, t) * 2 + core, p)
                    line_copy(way, t + 1, n0 + i, ref).wait_send()
        if t + 1 < C - 1:
            loop(0, n1, passed)
        for way in range(2):
            @pl.when(can_recv(way, t))
            def _(way=way, t=t):
                relayed(1 + way * (C - 1) + t, chip_of(way, t), True, rls)
    for k in range(B):
        for i in range(C):
            @pl.when(kbsends(k, 0, i) | (i == 0))
            def _(k=k, i=i):
                wait_all(kball.at[me, k], kbs.at[k, i])
            if i:
                kbrelay(k, i, True).wait_send()
        for t in range(C - 2):
            for way in range(2):
                @pl.when((sec > 0) & can_recv(way, t) & can_send(way, t + 1))
                def _(k=k, t=t, way=way):
                    kbpass(k, way, t).wait_send()

    @pl.when(sec < S - 1)
    def _():
        for k in range(B):
            sent(k)

    @pl.when((sec == S - 1) & (core == 1))
    def _():
        sent(B - 1)


def body(S, N, inputs, cotangent, norm_gain, key_weight, value_weight, plan):
    B, L, D = inputs.shape[1:]
    w, KV = key_weight.shape[1:]
    KH = KV // HEAD_DIM
    CW = D // KH
    G = CW // HEAD_DIM
    C = N // 2
    slots = line_slots(S, w)
    units = shares(S, w)[0]
    cos, sin = rope_tables(L)
    gain8 = jnp.broadcast_to(norm_gain.astype(F32), (8, w))
    vmem = pl.BlockSpec(memory_space=pltpu.VMEM)
    hbm = pl.BlockSpec(memory_space=pl.ANY)
    dma = pltpu.SemaphoreType.DMA
    low, gk, gv, gg = pl.pallas_call(
        functools.partial(kernel, S, N),
        out_shape=(
            jax.ShapeDtypeStruct((B * L, D), BF16),
            jax.ShapeDtypeStruct((w, KV), F32),
            jax.ShapeDtypeStruct((w, KV), F32),
            jax.ShapeDtypeStruct((8, w), F32),
        ),
        in_specs=[vmem, hbm, vmem, hbm, hbm, vmem, vmem],
        out_specs=(vmem,) * 4,
        scratch_shapes=[
            pltpu.VMEM((N, w, 2 * KV), BF16),
            pltpu.VMEM((N, B * L, w), BF16),
            pltpu.VMEM((N, B * L, w), BF16),
            pltpu.VMEM((N, 8, w), F32),
            pltpu.VMEM((B * L, 128), F32),
            pltpu.VMEM((B * L, 2 * KV), F32),
            pltpu.VMEM((B, KH, L, HEAD_DIM), BF16),
            pltpu.VMEM((B, KH, L, HEAD_DIM), BF16),
            pltpu.VMEM((B, KH, G * L, HEAD_DIM), BF16),
            pltpu.VMEM((B, KH, G * L, L), F32),
            pltpu.VMEM((B, KH, L, CW), BF16),
            pltpu.VMEM((B, KH, L, CW), BF16),
            pltpu.VMEM((N, L, w), F32),
            pltpu.VMEM((N, B, KH, L, 2 * HEAD_DIM), BF16),
            pltpu.VMEM((N, 8, w), F32),
            pltpu.VMEM((N, 8, w), F32),
            pltpu.VMEM((C, slots, w // units, 2 * KV), BF16),
            dma((2,)),
            dma((2, C - 1, slots)),
            dma((2, C - 1, slots)),
            dma((2, 2, C - 1, slots)),
            dma((2, C - 1, units)),
            dma((units,)),
            dma((slots,)),
            pltpu.SemaphoreType.REGULAR,
            pltpu.SemaphoreType.REGULAR,
            dma((2 * C - 1,)),
            dma((2 * C - 1,)),
            dma((2,)),
            dma((2,)),
            dma((2,)),
            dma((B, KH)),
            dma((B, KH)),
            dma((B, KH)),
            dma((B, C)),
            dma((B, C)),
            dma((B, C)),
            dma((B, C)),
            dma((B, 2, max(C - 2, 1))),
        ],
        compiler_params=pltpu.CompilerParams(
            collective_id=0, has_side_effects=True, vmem_limit_bytes=56 * 1024 * 1024),
    )(inputs[0].reshape(B * L, D), cotangent, gain8, key_weight[0], value_weight[0],
      jnp.asarray(cos), jnp.asarray(sin))
    low = low.reshape(B, L, D)
    selector = plan[0][:, None] == jnp.arange(B, dtype=jnp.int32)[None, :]
    ordered = jnp.sum(
        jnp.where(selector[:, :, None, None], low[None], jnp.zeros((), BF16)), axis=1)
    return ordered[None], gk[None], gv[None], gg[0:1]


def solution(mesh):
    in_specs = (
        P("section", None, "dp", None),
        P(None, "dp", None),
        P("section", "dp"),
        P("section", "dp", None),
        P("section", "dp", None),
        P("section", None),
    )
    out_specs = (
        P("section", None, "dp", None),
        P("section", "dp", None),
        P("section", "dp", None),
        P("section", "dp"),
    )
    run = functools.partial(body, mesh.shape["section"], mesh.shape["dp"])
    return jax.shard_map(run, mesh=mesh, in_specs=in_specs, out_specs=out_specs, check_vma=False)
```

```python
import functools
import math

import jax
import jax.numpy as jnp
import numpy as np
from jax import lax
from jax.experimental import pallas as pl
from jax.experimental.pallas import tpu as pltpu
from jax.sharding import PartitionSpec as P

HEAD_DIM = 128
EPS = 1e-05
ROPE_BASE = 500000.0
DIRECT = (9, 12, 8, 10)
ACROSS = (7, 4, 8, 4)
NS0 = 2
NS1 = 2
KB0 = 1
J3T = 0
J3H = 0
MESH = pl.DeviceIdType.MESH
F32 = jnp.float32
BF16 = jnp.bfloat16


def dot_nn(a, b):
    return lax.dot_general(a, b, (((1,), (0,)), ((), ())), preferred_element_type=F32)


def dot_nt(a, b):
    return lax.dot_general(a, b, (((1,), (1,)), ((), ())), preferred_element_type=F32)


def dot_tn(a, b):
    return lax.dot_general(a, b, (((0,), (0,)), ((), ())), preferred_element_type=F32)


def rope_tables(length):
    half = HEAD_DIM // 2
    freq = (ROPE_BASE ** (-(np.arange(half, dtype=np.float32) * 2.0 / HEAD_DIM))).astype(np.float32)
    angles = np.arange(length, dtype=np.float32)[:, None] * freq[None, :]
    cos, sin = np.cos(angles), np.sin(angles)
    return (
        np.concatenate([cos, cos], -1).astype(np.float32),
        np.concatenate([-sin, sin], -1).astype(np.float32),
    )


def shares(S, w):
    units = 16 if w % 256 == 0 else 8
    if S % 4:
        return units, False, (units,) * 4, (0,) * 4, (0,) * 4
    direct = tuple(d * units // 16 for d in DIRECT)
    across = tuple(a * units // 16 if r % 3 == 0 else units - direct[r] for r, a in enumerate(ACROSS))
    return units, True, direct, across, tuple(units - d - a for d, a in zip(direct, across))


def line_slots(S, w):
    units, shared, direct, across, near = shares(S, w)
    before = (across[2], across[3], near[3], 0)
    after = (0, near[0], across[0], across[1])
    return max(before[r] + direct[r] + after[r] for r in range(4))


def kernel(S, N, x_hbm, cot_ref, gain_hbm, wk_ref, wv_ref, cos_hbm, sin_hbm,
           low_out, rows_out, back_out, gg_out,
           x_ref, gain_ref, cos_ref, sin_ref, wall, ns, nall, gall, inv_s, acc, key_s, val_s, qst, prob, ubuf, lowb, gnb,
           kball, gsh, gsall, stage,
           loc, ws, wr, hs, hr, es, er, token, release, rls, rlr, gsem, nsem, ssem, us, ur, uloc, kbs, kbr, krs, krr, kfs, lsem, osem):
    B, KH, L = ubuf.shape[0], ubuf.shape[1], ubuf.shape[2]
    CW = ubuf.shape[3]
    w = wall.shape[1]
    KV = KH * HEAD_DIM
    G = CW // HEAD_DIM
    D = x_ref.shape[1]
    C = N // 2
    scale = 1.0 / math.sqrt(HEAD_DIM)
    sec = lax.axis_index("section")
    me = lax.axis_index("dp")
    c = me // 2
    core = me % 2
    partner = c * 2 + (1 - core)
    role = sec % 4
    UNITS, shared, direct, across, near = shares(S, w)
    hp = w // UNITS

    def by_role(values):
        out = jnp.int32(values[3])
        for r in range(3):
            out = jnp.where(role == r, jnp.int32(values[r]), out)
        return out

    up = role >= 2
    pair = jnp.where(up, sec - 2, sec + 2) if shared else sec
    first = (direct[2], direct[3], direct[3] + across[3], 0)
    counts = (across[2], across[3], near[3], 0)
    lo0, n0 = by_role(first), by_role(counts)
    n1 = by_role(direct)
    n2 = by_role((0, 0, across[0], across[1] * J3H))
    lo2 = by_role((0, 0, direct[0], direct[1]))
    n3 = by_role((0, near[0], 0, across[1] * (1 - J3H)))
    lo3 = by_role((0, direct[0] + across[0], 0, direct[1]))
    owner3 = jnp.where(role == 1, sec - 1, pair)
    owner0 = jnp.where(role == 2, sec + 1, pair)

    def remote(src, dst, send, recv, peer):
        return pltpu.make_async_remote_copy(
            src_ref=src, dst_ref=dst, send_sem=send, recv_sem=recv,
            device_id=(sec, peer), device_id_type=MESH)

    def wait_all(ref, sem):
        pltpu.make_async_copy(ref, ref, sem).wait()

    ck = pltpu.make_async_copy(wk_ref, wall.at[me, :, pl.ds(0, KV)], loc.at[0])
    cv = pltpu.make_async_copy(wv_ref, wall.at[me, :, pl.ds(KV, KV)], loc.at[1])
    small = [
        pltpu.make_async_copy(src, dst, loc.at[2 + i])
        for i, (src, dst) in enumerate((
            (gain_hbm, gain_ref), (x_hbm, x_ref), (cos_hbm, cos_ref), (sin_hbm, sin_ref)))]
    small[0].start()
    ck.start()
    cv.start()
    for cp in small[1:]:
        cp.start()

    barrier = pltpu.get_barrier_semaphore()
    for i in range(1, N):
        pl.semaphore_signal(barrier, inc=1, device_id=(sec, (me + i) % N), device_id_type=MESH)

    @pl.when(sec > 0)
    def _():
        pl.semaphore_signal(barrier, inc=1, device_id=(sec - 1, me), device_id_type=MESH)

    @pl.when(sec < S - 1)
    def _():
        pl.semaphore_signal(barrier, inc=1, device_id=(sec + 1, me), device_id_type=MESH)
    if shared:
        first_sec = sec - role
        for step in range(1, 4):
            for i in range(C):
                pl.semaphore_signal(
                    barrier, inc=1, device_id=(first_sec + (role + step) % 4, i * 2 + core),
                    device_id_type=MESH)
    below = jnp.where(sec > 0, 1, 0)
    above = jnp.where(sec < S - 1, 1, 0)
    pl.semaphore_wait(barrier, N - 1 + below + above + (3 * C if shared else 0))

    small[0].wait()
    gall[me] = jnp.broadcast_to(gain_ref[...].astype(F32), gall.shape[1:])
    gcopies = []
    for i in range(1, N):
        cp = remote(gall.at[me], gall.at[me], gsem.at[0], gsem.at[1], (me + i) % N)
        cp.start()
        gcopies.append(cp)
    ck.wait()
    cv.wait()

    def piece(shard, p):
        return wall.at[shard, pl.ds(p * hp, hp)]

    def chip_of(way, t):
        return c - 1 - t if way == 0 else c + 1 + t

    def line_copy(way, t, v, ref):
        peer = (c + 1 if way == 0 else c - 1) * 2 + core
        return remote(ref, ref, ws.at[way, t, v], wr.at[way, t, v], peer)

    def relay(slot, chip, p, mine):
        ref = piece(chip * 2 + (core if mine else 1 - core), p)
        return remote(ref, ref, rls.at[slot], rlr.at[slot], partner)

    def relayed(slot, chip, mine, sem):
        wait_all(wall.at[chip * 2 + (core if mine else 1 - core)], sem.at[slot])

    def enter(p, v, helper):
        return pltpu.make_async_remote_copy(
            src_ref=piece(me, p), dst_ref=stage.at[c, v], send_sem=es.at[p],
            recv_sem=er.at[v], device_id=(helper, me), device_id_type=MESH)

    def deliver(way, chip, kind, t, v, p, owner):
        peer = (chip + t + 1 if way == 0 else chip - t - 1) * 2 + core
        return pltpu.make_async_remote_copy(
            src_ref=stage.at[chip, v], dst_ref=piece(chip * 2 + core, p),
            send_sem=hs.at[kind, way, t, v], recv_sem=hr.at[way, t, p],
            device_id=(owner, peer), device_id_type=MESH)

    def relay_on(way, chip, t, v):
        peer = (chip + t + 1 if way == 0 else chip - t - 1) * 2 + core
        ref = stage.at[chip, v]
        return remote(ref, ref, ws.at[way, t, v], wr.at[way, t, v], peer)

    def can_send(way, t):
        return ((c - t >= 0) & (c + 1 < C)) if way == 0 else ((c + t < C) & (c >= 1))

    def can_recv(way, t):
        return (c - 1 - t >= 0) if way == 0 else (c + 1 + t < C)

    def loop(lo, n, f):
        def step(i, carry):
            f(lo + i, i)
            return carry
        lax.fori_loop(0, n, step, 0)

    JOBS = (
        (lo0, n0, 0, owner0),
        (lo2, n2, n0 + n1, pair),
        (lo3, n3, n0 + n1, owner3),
    )

    def left_over(way):
        return C - 1 - c if way == 0 else c

    def spread_far(way, chip, a, v, act):
        @pl.when(left_over(way) >= 3)
        def _():
            act(relay_on(way, chip, a + 1, v))

    def spread_near(way, chip, a, v, p, owner, act):
        left = left_over(way)

        @pl.when(left == 2)
        def _():
            act(deliver(way, chip, 0, a + 1, v, p, owner))

        @pl.when(left >= 1)
        def _():
            act(deliver(way, chip, 0, a, v, p, owner))

    def spread(way, chip, a, v, p, owner, act):
        spread_far(way, chip, a, v, act)
        spread_near(way, chip, a, v, p, owner, act)

    far_end = (left_over(0) >= 3) | (left_over(1) >= 3)

    def start(copy):
        copy.start()

    def sent_out(copy):
        copy.wait_send()

    def own_sends(act):
        def one(p, i):
            for way in range(2):
                @pl.when(can_send(way, 0))
                def _(way=way):
                    act(line_copy(way, 0, n0 + i, piece(c * 2 + core, p)))
        loop(0, n1, one)

    def help_far(job, act, arrive):
        lo, n, at, owner = JOBS[job]

        def one(p, i):
            @pl.when(far_end)
            def _():
                if arrive:
                    enter(p, at + i, owner).wait_recv()
                for way in range(2):
                    spread_far(way, c, 0, at + i, act)
        loop(lo, n, one)

    def help_near(job, act, arrive):
        lo, n, at, owner = JOBS[job]

        def one(p, i):
            if arrive:
                @pl.when(jnp.logical_not(far_end))
                def _():
                    enter(p, at + i, owner).wait_recv()
            for way in range(2):
                spread_near(way, c, 0, at + i, p, owner, act)
        loop(lo, n, one)

    def help_on(job, act, arrive):
        lo, n, at, owner = JOBS[job]
        for t in range(1, C - 1, 2):
            def one(p, i, t=t):
                v = at + i
                for way in range(2):
                    @pl.when(can_recv(way, t) & (left_over(way) >= 1))
                    def _(way=way):
                        chip = chip_of(way, t)
                        if arrive:
                            relay_on(way, chip, t, v).wait_recv()
                        spread(way, chip, t + 1, v, p, owner, act)
                        act(deliver(way, chip, 1, t, v, p, owner))
            loop(lo, n, one)

    def help_direct(job, act, arrive):
        lo, n, at, owner = JOBS[job]

        def one(p, i):
            if arrive:
                enter(p, at + i, owner).wait_recv()
            for way in range(2):
                for t in reversed(range(C - 1)):
                    @pl.when(left_over(way) > t)
                    def _(way=way, t=t):
                        act(deliver(way, c, 0, t, at + i, p, owner))
        loop(lo, n, one)

    def serve(t):
        def one(p, i):
            v = n0 + i
            for way in range(2):
                @pl.when(can_recv(way, t))
                def _(way=way):
                    chip = chip_of(way, t)
                    ref = piece(chip * 2 + core, p)
                    line_copy(way, t, v, ref).wait_recv()
                    if t + 1 < C - 1:
                        @pl.when(can_send(way, t + 1))
                        def _():
                            line_copy(way, t + 1, v, ref).start()
                    relay(1 + way * (C - 1) + t, chip, p, True).start()
        loop(0, n1, one)

    def handed(t):
        def one(p, i):
            for way in range(2):
                @pl.when(can_recv(way, t))
                def _(way=way):
                    chip = chip_of(way, t)
                    ref = piece(chip * 2 + core, p)
                    remote(ref, ref, hs.at[way, t, 0], hr.at[way, t, p], partner).wait_recv()
                    relay(1 + way * (C - 1) + t, chip, p, True).start()
        loop(n1, UNITS - n1, one)

    def enter_all(act):
        if not shared:
            return
        far = by_role((near[3] + direct[2], direct[3], 0, 0))

        def one(p, i):
            act(enter(p, far + i, pair))
        loop(n1, by_role(across), one)
        for r, at, step in ((3, 0, -1), (0, across[3] + direct[1], 1)):
            @pl.when(role == r)
            def _(r=r, at=at, step=step):
                def other(p, i):
                    act(enter(p, at + i, sec + step))
                loop(direct[r] + across[r], near[r], other)

    enter_all(start)

    @pl.when(n0 == 0)
    def _():
        own_sends(start)
    remote(wall.at[me], wall.at[me], rls.at[0], rlr.at[0], partner).start()
    help_far(0, start, True)
    help_near(0, start, True)

    def cot_copy(k, j):
        return pltpu.make_async_copy(
            cot_ref.at[k, :, pl.ds(j * CW, CW)], ubuf.at[k, j], uloc.at[k, j])

    @pl.when(sec == S - 1)
    def _():
        for k in range(B):
            for j in range(KH):
                cot_copy(k, j).start()

    for cp in small[1:]:
        cp.wait()
    total = jnp.zeros((B * L, 1), F32)
    for d in range(N):
        xd = x_ref[:, d * w:(d + 1) * w].astype(F32)
        total = total + jnp.sum(xd * xd, axis=-1, keepdims=True)
    inv = lax.rsqrt(total * (1.0 / D) + EPS)
    inv_s[...] = jnp.broadcast_to(inv, inv_s.shape)
    wait_all(gall.at[pl.ds(0, N - 1)], gsem.at[1])
    for d in range(N):
        xd = x_ref[:, d * w:(d + 1) * w].astype(F32)
        ns[d] = (xd * inv * gall[d][0:1, :]).astype(BF16)
        gsh[d] = jnp.zeros(gsh.shape[1:], F32)
    nall[me] = ns[me]
    cos = cos_ref[...]
    sin = sin_ref[...]

    def queries(k, carry):
        rows = pl.ds(pl.multiple_of(k * L, L), L)
        for j in range(KH):
            for g in range(G):
                col = (j * G + g) * HEAD_DIM
                v = ns[col // w, rows, col % w:col % w + HEAD_DIM].astype(F32)
                q = v * cos + pltpu.roll(v, HEAD_DIM // 2, 1) * sin
                qst[k, j, g * L:(g + 1) * L, :] = q.astype(BF16)
        return carry
    lax.fori_loop(0, B, queries, 0)

    def use_step(t):
        for way in range(2):
            @pl.when(can_recv(way, t))
            def _(way=way):
                chip = c - 1 - t if way == 0 else c + 1 + t
                relayed(1 + way * (C - 1) + t, chip, False, rlr)
                acc[...] += dot_nn(ns[chip * 2], wall[chip * 2]) + dot_nn(
                    ns[chip * 2 + 1], wall[chip * 2 + 1])

    help_on(0, start, True)

    def send_rows():
        for i in range(1, N):
            peer = (me + i) % N
            remote(ns.at[peer], nall.at[me], nsem.at[0], nsem.at[1], peer).start()

    @pl.when((role == 0) & (n0 > 0) & (NS0 == 0))
    def _():
        send_rows()

    @pl.when(n0 > 0)
    def _():
        own_sends(start)
    relayed(0, c, False, rlr)
    acc[...] = dot_nn(ns[c * 2], wall[c * 2]) + dot_nn(ns[c * 2 + 1], wall[c * 2 + 1])
    for t in range(C - 1):
        serve(t)
        if t == max(C - 3, 0):
            help_far(1, start, True)
        if 0 < t < C - 2:
            handed(t - 1)
    help_near(1, start, True)

    @pl.when((role < 3) | (J3T == 0))
    def _():
        help_direct(2, start, True)

    @pl.when(((role == 0) & (NS0 == 2)) | ((role == 1) & (NS1 == 2)))
    def _():
        send_rows()

    if C > 2:
        handed(C - 3)
    for t in range(C - 2):
        use_step(t)
    handed(C - 2)
    use_step(C - 2)

    row_pos = lax.broadcasted_iota(jnp.int32, (L, L), 0)
    col_pos = lax.broadcasted_iota(jnp.int32, (L, L), 1)
    causal = (row_pos >= col_pos)[None]

    def attend(k, carry):
        rows = pl.ds(pl.multiple_of(k * L, L), L)
        for j in range(KH):
            kp = acc[rows, j * HEAD_DIM:(j + 1) * HEAD_DIM]
            key = (kp * cos + pltpu.roll(kp, HEAD_DIM // 2, 1) * sin).astype(BF16)
            key_s[k, j] = key
            val_s[k, j] = acc[rows, KV + j * HEAD_DIM:KV + (j + 1) * HEAD_DIM].astype(BF16)
            sc = dot_nt(qst[k, j], key) * scale
            raised = jnp.where(causal, jnp.exp(sc.reshape(G, L, L)), 0.0)
            pr = raised / jnp.sum(raised, axis=-1, keepdims=True)
            prob[k, j] = pr.reshape(G * L, L)
        return carry
    lax.fori_loop(0, B, attend, 0)

    half = C // 2

    def in_turn(outward):
        first = jnp.where(c < half, half - 1 if outward else 0, half if outward else C - 1)
        last = jnp.where(c < half, 0 if outward else half - 1, C - 1 if outward else half)
        away = jnp.where((c < half) == outward, -2, 2)

        @pl.when(c != first)
        def _():
            pl.semaphore_wait(release, 1)

        @pl.when(c != last)
        def _():
            pl.semaphore_signal(
                release, inc=1, device_id=(sec, me + away), device_id_type=MESH)

    @pl.when(((role == 1) & (NS1 == 0)) | ((role == 0) & (NS0 == 1)))
    def _():
        in_turn(False)
        send_rows()

    def usend(k, j):
        return pltpu.make_async_remote_copy(
            src_ref=lowb.at[k, j], dst_ref=ubuf.at[k, j], send_sem=us.at[k, j],
            recv_sem=ur.at[k, j], device_id=(lax.max(sec - 1, 0), me), device_id_type=MESH)

    def kbcopy(k, j, i):
        peer = ((c + i) % C) * 2 + core
        ref = kball.at[me, k, j]
        return remote(ref, ref, kbs.at[k, i], kbr.at[k, i], peer)

    def kbpartner(k, j):
        ref = kball.at[me, k, j]
        return remote(ref, ref, kbs.at[k, 0], kbr.at[k, 0], partner)

    def kbsends(k, j, i):
        right = (i == 1) & (c + 1 < C)
        left = (i == C - 1) & (c >= 1)
        return ((sec == 0) & (KB0 == 1)) | right | left

    def kbshare(k, j):
        kbpartner(k, j).start()
        for i in range(1, C):
            @pl.when(kbsends(k, j, i))
            def _(i=i):
                kbcopy(k, j, i).start()

    def from_chip(way, t):
        return t + 1 if way == 0 else C - 1 - t

    def kbpass(k, way, t):
        ref = kball.at[chip_of(way, t) * 2 + core, k]
        peer = (c + 1 if way == 0 else c - 1) * 2 + core
        return remote(ref, ref, kfs.at[k, way, t], kbr.at[k, from_chip(way, t + 1)], peer)

    def kbrelay(k, i, mine):
        chip = (c - i + C) % C
        ref = kball.at[chip * 2 + (core if mine else 1 - core), k]
        return remote(ref, ref, krs.at[k, i], krr.at[k, i], partner)

    def sent(k):
        @pl.when(sec > 0)
        def _():
            for j in range(KH):
                usend(k, j).wait_send()

    def low_copy(k, j):
        rows = pl.ds(pl.multiple_of(k * L, L), L)
        return pltpu.make_async_copy(
            lowb.at[k, j], low_out.at[rows, pl.ds(j * CW, CW)], lsem.at[k, j])

    def turn(k, carry):
        rows = pl.ds(pl.multiple_of(k * L, L), L)
        keys, values = [], []
        along = jnp.zeros((L, HEAD_DIM), F32)

        @pl.when((k == B - 1) & (role >= 2))
        def _():
            help_on(1, start, True)
            if J3T == 1:
                @pl.when(role == 3)
                def _():
                    help_direct(2, start, True)
        for j in range(KH):
            @pl.when(sec == S - 1)
            def _(j=j):
                cot_copy(k, j).wait()

            @pl.when(sec < S - 1)
            def _(j=j):
                usend(k, j).wait_recv()
            u = ubuf[k, j]
            us_ = jnp.concatenate(
                [u[:, g * HEAD_DIM:(g + 1) * HEAD_DIM] for g in range(G)], axis=0)
            key, q, pr = key_s[k, j], qst[k, j], prob[k, j]
            gp = dot_nt(us_, val_s[k, j])
            gv = dot_tn(pr.astype(BF16), us_).astype(BF16)
            rd = jnp.sum(pr * gp, axis=-1, keepdims=True)
            gs = (pr * (gp - rd) * scale).astype(BF16)
            gk = dot_tn(gs, q)
            gk = (gk * cos - pltpu.roll(gk, HEAD_DIM // 2, 1) * sin).astype(BF16)
            keys.append(gk)
            values.append(gv)
            kball[me, k, j] = jnp.concatenate([gk, gv], axis=1)
            gq = dot_nn(gs, key)
            at = j * HEAD_DIM
            along = along + gk.astype(F32) * acc[rows, at:at + HEAD_DIM]
            along = along + gv.astype(F32) * acc[rows, KV + at:KV + at + HEAD_DIM]
            for g in range(G):
                v = gq[g * L:(g + 1) * L]
                along = along + v * q[g * L:(g + 1) * L].astype(F32)
                col = (j * G + g) * HEAD_DIM
                gnb[col // w, :, col % w:col % w + HEAD_DIM] = (
                    v * cos - pltpu.roll(v, HEAD_DIM // 2, 1) * sin)
            @pl.when(sec == 0)
            def _(j=j):
                kbshare(k, j)
        @pl.when((sec == S - 1) & (k > 0))
        def _():
            sent(k - 1)
            pl.semaphore_signal(token, inc=1, device_id=(sec, partner), device_id_type=MESH)
        kbv = jnp.concatenate(keys + values, axis=1)
        part_inv = inv_s[rows, 0:1]
        proj = jnp.sum(along, axis=-1, keepdims=True) * (1.0 / D) * part_inv * part_inv
        for j in range(KH):
            for e in range(N // KH):
                d = j * (N // KH) + e
                gn = gnb[d] + dot_nt(kbv, wall[d])
                xd = x_ref[rows, d * w:(d + 1) * w].astype(F32)
                gt = gn * xd * part_inv
                gsh[d] += jnp.sum(gt.reshape(L // 8, 8, w), axis=0)
                u = ubuf[k, j, :, e * w:(e + 1) * w].astype(F32)
                low = (u + part_inv * gall[d][0:1, :] * gn - xd * proj).astype(BF16)
                lowb[k, j, :, e * w:(e + 1) * w] = low
            if j == 0:
                @pl.when((sec == S - 1) & ((k > 0) | (core > 0)))
                def _():
                    pl.semaphore_wait(token, 1)

            low_copy(k, j).start()

            @pl.when(sec > 0)
            def _(j=j):
                usend(k, j).start()
        return carry
    lax.fori_loop(0, B, turn, 0)

    help_direct(2, sent_out, False)
    for job in range(2):
        help_far(job, sent_out, False)
        help_near(job, sent_out, False)
        help_on(job, sent_out, False)
    @pl.when(role >= 2)
    def _():
        in_turn(True)

    @pl.when((role >= 2) | ((role == 0) & (n0 == 0) & (NS0 == 0)) | ((role == 1) & (NS1 == 1)))
    def _():
        send_rows()

    @pl.when(sec > 0)
    def _():
        for k in range(B):
            for j in range(KH):
                kbshare(k, j)

    relayed(0, c, True, rls)
    enter_all(sent_out)
    own_sends(sent_out)
    for t in range(C - 1):
        def passed(p, i, t=t):
            for way in range(2):
                @pl.when(can_recv(way, t) & can_send(way, t + 1))
                def _(way=way):
                    ref = piece(chip_of(way, t) * 2 + core, p)
                    line_copy(way, t + 1, n0 + i, ref).wait_send()
        if t + 1 < C - 1:
            loop(0, n1, passed)
        for way in range(2):
            @pl.when(can_recv(way, t))
            def _(way=way, t=t):
                relayed(1 + way * (C - 1) + t, chip_of(way, t), True, rls)

    @pl.when((sec == S - 1) & (core == 0))
    def _():
        sent(B - 1)
        pl.semaphore_signal(token, inc=1, device_id=(sec, partner), device_id_type=MESH)

    gsall[me] = gsh[me]
    for i in range(1, N):
        peer = (me + i) % N
        remote(gsh.at[peer], gsall.at[me], ssem.at[0], ssem.at[1], peer).start()
    for k in range(B):
        for t in range(C - 1):
            for way in range(2):
                @pl.when(can_recv(way, t))
                def _(k=k, t=t, way=way):
                    i = from_chip(way, t)
                    wait_all(kball.at[chip_of(way, t) * 2 + core, k], kbr.at[k, i])
                    if t + 1 < C - 1:
                        @pl.when(((sec > 0) | (KB0 == 0)) & can_send(way, t + 1))
                        def _():
                            kbpass(k, way, t).start()
                    kbrelay(k, i, True).start()
    wait_all(nall.at[pl.ds(0, N - 1)], nsem.at[1])
    outs = [pltpu.make_async_copy(nall, rows_out, osem.at[B])]
    outs[0].start()
    for k in range(B):
        wait_all(kball.at[partner, k], kbr.at[k, 0])
        for i in range(1, C):
            kbrelay(k, i, False).wait_recv()
        cp = pltpu.make_async_copy(kball.at[:, k], back_out.at[:, k], osem.at[k])
        cp.start()
        outs.append(cp)
    wait_all(gsall.at[pl.ds(0, N - 1)], ssem.at[1])
    gg = gsall[0]
    for d in range(1, N):
        gg = gg + gsall[d]
    gg_out[...] = jnp.sum(gg, axis=0, keepdims=True)
    for k in range(B):
        for j in range(KH):
            low_copy(k, j).wait()

    wait_all(gall.at[pl.ds(0, N - 1)], gsem.at[0])
    wait_all(nall.at[pl.ds(0, N - 1)], nsem.at[0])
    wait_all(gsall.at[pl.ds(0, N - 1)], ssem.at[0])
    for k in range(B):
        for i in range(C):
            @pl.when(kbsends(k, 0, i) | (i == 0))
            def _(k=k, i=i):
                wait_all(kball.at[me, k], kbs.at[k, i])
            if i:
                kbrelay(k, i, True).wait_send()
        for t in range(C - 2):
            for way in range(2):
                @pl.when(((sec > 0) | (KB0 == 0)) & can_recv(way, t) & can_send(way, t + 1))
                def _(k=k, t=t, way=way):
                    kbpass(k, way, t).wait_send()

    @pl.when(sec < S - 1)
    def _():
        for k in range(B):
            sent(k)

    @pl.when((sec == S - 1) & (core == 1))
    def _():
        sent(B - 1)
    for cp in outs:
        cp.wait()


def finish(plan_ref, low_ref, rows_ref, back_ref, gg_ref, low_out, gk_out, gv_out, gg_out,
           low_s, rows_s, back_s, held, lsem, isem, gsem):
    N, B, KH, L = back_ref.shape[:4]
    w = rows_ref.shape[2]
    fetch_rows = pltpu.make_async_copy(rows_ref, rows_s, isem.at[KH])
    fetch_back = [
        pltpu.make_async_copy(back_ref.at[:, :, j], back_s.at[:, :, j], isem.at[j])
        for j in range(KH)]
    fetch_low = [
        pltpu.make_async_copy(
            low_ref.at[pl.ds(pl.multiple_of(plan_ref[0, k] * L, L), L)], low_s.at[k], lsem.at[0, k])
        for k in range(B)]
    fetch_rows.start()
    for cp in fetch_back + fetch_low:
        cp.start()
    gg_out[...] = gg_ref[...]
    fetch_rows.wait()
    rows_all = rows_s[...].reshape(N * B * L, w)
    copies = []
    for j in range(KH):
        fetch_back[j].wait()
        back = jnp.concatenate(
            [back_s[g, k, j] for g in range(N) for k in range(B)], axis=0)
        dw = dot_tn(rows_all, back)
        for i, out in enumerate((gk_out, gv_out)):
            held[i, j] = dw[:, i * HEAD_DIM:(i + 1) * HEAD_DIM]
            copies.append(pltpu.make_async_copy(
                held.at[i, j], out.at[0, :, pl.ds(j * HEAD_DIM, HEAD_DIM)], gsem.at[i, j]))
            copies[-1].start()
        if j == 0:
            for k in range(B):
                fetch_low[k].wait()
                copies.append(pltpu.make_async_copy(low_s.at[k], low_out.at[0, k], lsem.at[1, k]))
                copies[-1].start()
    for cp in copies:
        cp.wait()


def body(S, N, inputs, cotangent, norm_gain, key_weight, value_weight, plan):
    B, L, D = inputs.shape[1:]
    w, KV = key_weight.shape[1:]
    KH = KV // HEAD_DIM
    CW = D // KH
    G = CW // HEAD_DIM
    C = N // 2
    slots = line_slots(S, w)
    units = shares(S, w)[0]
    cos, sin = rope_tables(L)
    vmem = pl.BlockSpec(memory_space=pltpu.VMEM)
    hbm = pl.BlockSpec(memory_space=pl.ANY)
    dma = pltpu.SemaphoreType.DMA
    low, rows, back, gg = pl.pallas_call(
        functools.partial(kernel, S, N),
        out_shape=(
            jax.ShapeDtypeStruct((B * L, D), BF16),
            jax.ShapeDtypeStruct((N, B * L, w), BF16),
            jax.ShapeDtypeStruct((N, B, KH, L, 2 * HEAD_DIM), BF16),
            jax.ShapeDtypeStruct((1, w), F32),
        ),
        in_specs=[hbm] * 7,
        out_specs=(hbm, hbm, hbm, vmem),
        scratch_shapes=[
            pltpu.VMEM((B * L, D), BF16),
            pltpu.VMEM((1, w), BF16),
            pltpu.VMEM((L, HEAD_DIM), F32),
            pltpu.VMEM((L, HEAD_DIM), F32),
            pltpu.VMEM((N, w, 2 * KV), BF16),
            pltpu.VMEM((N, B * L, w), BF16),
            pltpu.VMEM((N, B * L, w), BF16),
            pltpu.VMEM((N, 8, w), F32),
            pltpu.VMEM((B * L, 128), F32),
            pltpu.VMEM((B * L, 2 * KV), F32),
            pltpu.VMEM((B, KH, L, HEAD_DIM), BF16),
            pltpu.VMEM((B, KH, L, HEAD_DIM), BF16),
            pltpu.VMEM((B, KH, G * L, HEAD_DIM), BF16),
            pltpu.VMEM((B, KH, G * L, L), F32),
            pltpu.VMEM((B, KH, L, CW), BF16),
            pltpu.VMEM((B, KH, L, CW), BF16),
            pltpu.VMEM((N, L, w), F32),
            pltpu.VMEM((N, B, KH, L, 2 * HEAD_DIM), BF16),
            pltpu.VMEM((N, 8, w), F32),
            pltpu.VMEM((N, 8, w), F32),
            pltpu.VMEM((C, slots, w // units, 2 * KV), BF16),
            dma((6,)),
            dma((2, C - 1, slots)),
            dma((2, C - 1, slots)),
            dma((2, 2, C - 1, slots)),
            dma((2, C - 1, units)),
            dma((units,)),
            dma((slots,)),
            pltpu.SemaphoreType.REGULAR,
            pltpu.SemaphoreType.REGULAR,
            dma((2 * C - 1,)),
            dma((2 * C - 1,)),
            dma((2,)),
            dma((2,)),
            dma((2,)),
            dma((B, KH)),
            dma((B, KH)),
            dma((B, KH)),
            dma((B, C)),
            dma((B, C)),
            dma((B, C)),
            dma((B, C)),
            dma((B, 2, max(C - 2, 1))),
            dma((B, KH)),
            dma((B + 1,)),
        ],
        compiler_params=pltpu.CompilerParams(
            collective_id=0, has_side_effects=True, vmem_limit_bytes=56 * 1024 * 1024),
    )(inputs[0].reshape(B * L, D), cotangent, norm_gain, key_weight[0], value_weight[0],
      jnp.asarray(cos), jnp.asarray(sin))
    ordered, gk, gv, gg = pl.pallas_call(
        finish,
        out_shape=(
            jax.ShapeDtypeStruct((1, B, L, D), BF16),
            jax.ShapeDtypeStruct((1, w, KV), F32),
            jax.ShapeDtypeStruct((1, w, KV), F32),
            jax.ShapeDtypeStruct((1, w), F32),
        ),
        in_specs=[pl.BlockSpec(memory_space=pltpu.SMEM), hbm, hbm, hbm, vmem],
        out_specs=(hbm, hbm, hbm, vmem),
        scratch_shapes=[
            pltpu.VMEM((B, L, D), BF16),
            pltpu.VMEM((N, B * L, w), BF16),
            pltpu.VMEM((N, B, KH, L, 2 * HEAD_DIM), BF16),
            pltpu.VMEM((2, KH, w, HEAD_DIM), F32),
            dma((2, B)),
            dma((KH + 1,)),
            dma((2, KH)),
        ],
        compiler_params=pltpu.CompilerParams(vmem_limit_bytes=56 * 1024 * 1024),
    )(plan, low, rows, back, gg)
    return ordered, gk, gv, gg


def solution(mesh):
    in_specs = (
        P("section", None, "dp", None),
        P(None, "dp", None),
        P("section", "dp"),
        P("section", "dp", None),
        P("section", "dp", None),
        P("section", None),
    )
    out_specs = (
        P("section", None, "dp", None),
        P("section", "dp", None),
        P("section", "dp", None),
        P("section", "dp"),
    )
    run = functools.partial(body, mesh.shape["section"], mesh.shape["dp"])
    return jax.shard_map(run, mesh=mesh, in_specs=in_specs, out_specs=out_specs, check_vma=False)
```

```python
import functools
import math

import jax
import jax.numpy as jnp
import numpy as np
from jax import lax
from jax.experimental import pallas as pl
from jax.experimental.pallas import tpu as pltpu
from jax.sharding import PartitionSpec as P

HEAD_DIM = 128
EPS = 1e-05
ROPE_BASE = 500000.0
DIRECT = (9, 13, 8, 10)
ACROSS = (7, 3, 8, 4)
NS0 = 2
NS1 = 2
KB0 = 1
J3T = 0
MESH = pl.DeviceIdType.MESH
F32 = jnp.float32
BF16 = jnp.bfloat16


def dot_nn(a, b):
    return lax.dot_general(a, b, (((1,), (0,)), ((), ())), preferred_element_type=F32)


def dot_nt(a, b):
    return lax.dot_general(a, b, (((1,), (1,)), ((), ())), preferred_element_type=F32)


def dot_tn(a, b):
    return lax.dot_general(a, b, (((0,), (0,)), ((), ())), preferred_element_type=F32)


def rope_tables(length):
    half = HEAD_DIM // 2
    freq = (ROPE_BASE ** (-(np.arange(half, dtype=np.float32) * 2.0 / HEAD_DIM))).astype(np.float32)
    angles = np.arange(length, dtype=np.float32)[:, None] * freq[None, :]
    cos, sin = np.cos(angles), np.sin(angles)
    return (
        np.concatenate([cos, cos], -1).astype(np.float32),
        np.concatenate([-sin, sin], -1).astype(np.float32),
    )


def shares(S, w):
    units = 16 if w % 256 == 0 else 8
    if S % 4:
        return units, False, (units,) * 4, (0,) * 4, (0,) * 4
    direct = tuple(d * units // 16 for d in DIRECT)
    across = tuple(a * units // 16 if r % 3 == 0 else units - direct[r] for r, a in enumerate(ACROSS))
    return units, True, direct, across, tuple(units - d - a for d, a in zip(direct, across))


def line_slots(S, w):
    units, shared, direct, across, near = shares(S, w)
    before = (across[2], across[3], near[3], 0)
    after = (0, near[0], across[0], across[1])
    return max(1, max(before[r] + after[r] for r in range(4)))


def kernel(S, N, x_hbm, cot_ref, gain_hbm, wk_ref, wv_ref, cos_hbm, sin_hbm,
           low_out, rows_out, back_out, gg_out,
           x_ref, gain_ref, cos_ref, sin_ref, wall, ns, nall, gall, inv_s, acc, key_s, val_s, qst, prob, ubuf, lowb, gnb,
           kball, gsh, gsall, stage,
           loc, ws, wr, hs, ar, es, er, token, release, rls, rlr, gsem, nsem, ssem, us, ur, uloc, kbs, kbr, krs, krr, kfs, lsem, osem):
    B, KH, L = ubuf.shape[0], ubuf.shape[1], ubuf.shape[2]
    CW = ubuf.shape[3]
    w = wall.shape[1]
    KV = KH * HEAD_DIM
    G = CW // HEAD_DIM
    D = x_ref.shape[1]
    C = N // 2
    scale = 1.0 / math.sqrt(HEAD_DIM)
    sec = lax.axis_index("section")
    me = lax.axis_index("dp")
    c = me // 2
    core = me % 2
    partner = c * 2 + (1 - core)
    role = sec % 4
    UNITS, shared, direct, across, near = shares(S, w)
    hp = w // UNITS

    def by_role(values):
        out = jnp.int32(values[3])
        for r in range(3):
            out = jnp.where(role == r, jnp.int32(values[r]), out)
        return out

    up = role >= 2
    pair = jnp.where(up, sec - 2, sec + 2) if shared else sec
    first = (direct[2], direct[3], direct[3] + across[3], 0)
    counts = (across[2], across[3], near[3], 0)
    lo0, n0 = by_role(first), by_role(counts)
    n1 = by_role(direct)
    n2 = by_role((0, 0, across[0], 0))
    n3 = by_role((0, near[0], 0, across[1]))
    lo3 = by_role((0, direct[0] + across[0], 0, direct[1]))
    owner3 = jnp.where(role == 1, sec - 1, pair)
    owner0 = jnp.where(role == 2, sec + 1, pair)

    def remote(src, dst, send, recv, peer):
        return pltpu.make_async_remote_copy(
            src_ref=src, dst_ref=dst, send_sem=send, recv_sem=recv,
            device_id=(sec, peer), device_id_type=MESH)

    def wait_all(ref, sem):
        pltpu.make_async_copy(ref, ref, sem).wait()

    ck = pltpu.make_async_copy(wk_ref, wall.at[me, :, pl.ds(0, KV)], loc.at[0])
    cv = pltpu.make_async_copy(wv_ref, wall.at[me, :, pl.ds(KV, KV)], loc.at[1])
    small = [
        pltpu.make_async_copy(src, dst, loc.at[2 + i])
        for i, (src, dst) in enumerate((
            (gain_hbm, gain_ref), (x_hbm, x_ref), (cos_hbm, cos_ref), (sin_hbm, sin_ref)))]
    small[0].start()
    ck.start()
    cv.start()
    for cp in small[1:]:
        cp.start()

    barrier = pltpu.get_barrier_semaphore()
    for i in range(1, N):
        pl.semaphore_signal(barrier, inc=1, device_id=(sec, (me + i) % N), device_id_type=MESH)

    @pl.when(sec > 0)
    def _():
        pl.semaphore_signal(barrier, inc=1, device_id=(sec - 1, me), device_id_type=MESH)

    @pl.when(sec < S - 1)
    def _():
        pl.semaphore_signal(barrier, inc=1, device_id=(sec + 1, me), device_id_type=MESH)
    if shared:
        first_sec = sec - role
        for step in range(1, 4):
            for i in range(C):
                pl.semaphore_signal(
                    barrier, inc=1, device_id=(first_sec + (role + step) % 4, i * 2 + core),
                    device_id_type=MESH)
    below = jnp.where(sec > 0, 1, 0)
    above = jnp.where(sec < S - 1, 1, 0)
    pl.semaphore_wait(barrier, N - 1 + below + above + (3 * C if shared else 0))

    small[0].wait()
    gall[me] = jnp.broadcast_to(gain_ref[...].astype(F32), gall.shape[1:])
    gcopies = []
    for i in range(1, N):
        cp = remote(gall.at[me], gall.at[me], gsem.at[0], gsem.at[1], (me + i) % N)
        cp.start()
        gcopies.append(cp)
    ck.wait()
    cv.wait()

    def piece(shard, p):
        return wall.at[shard, pl.ds(p * hp, hp)]

    def chip_of(way, t):
        return c - 1 - t if way == 0 else c + 1 + t

    def line_copy(way, t, chip, p):
        peer = (c + 1 if way == 0 else c - 1) * 2 + core
        ref = piece(chip * 2 + core, p)
        return remote(ref, ref, ws.at[0, way, t], ar.at[chip, p], peer)

    def relay(slot, chip, p, mine):
        ref = piece(chip * 2 + (core if mine else 1 - core), p)
        return remote(ref, ref, rls.at[slot], rlr.at[slot], partner)

    def relayed(slot, chip, mine, sem):
        wait_all(wall.at[chip * 2 + (core if mine else 1 - core)], sem.at[slot])

    def enter(p, v, helper, kind=0):
        return pltpu.make_async_remote_copy(
            src_ref=piece(me, p), dst_ref=stage.at[c, v], send_sem=es.at[kind],
            recv_sem=er.at[v], device_id=(helper, me), device_id_type=MESH)

    def deliver(job, way, chip, kind, t, v, p, owner):
        peer = (chip + t + 1 if way == 0 else chip - t - 1) * 2 + core
        return pltpu.make_async_remote_copy(
            src_ref=stage.at[chip, v], dst_ref=piece(chip * 2 + core, p),
            send_sem=hs.at[min(job, 1), kind, way, t], recv_sem=ar.at[chip, p],
            device_id=(owner, peer), device_id_type=MESH)

    def relay_on(job, way, chip, t, v):
        peer = (chip + t + 1 if way == 0 else chip - t - 1) * 2 + core
        ref = stage.at[chip, v]
        return remote(ref, ref, ws.at[1 + job, way, t], wr.at[chip, v], peer)

    def can_send(way, t):
        return ((c - t >= 0) & (c + 1 < C)) if way == 0 else ((c + t < C) & (c >= 1))

    def can_recv(way, t):
        return (c - 1 - t >= 0) if way == 0 else (c + 1 + t < C)

    def loop(lo, n, f):
        def step(i, carry):
            f(lo + i, i)
            return carry
        lax.fori_loop(0, n, step, 0)

    JOBS = (
        (lo0, n0, 0, owner0),
        (direct[0], n2, n0, pair),
        (lo3, n3, n0, owner3),
    )

    def left_over(way):
        return C - 1 - c if way == 0 else c

    def spread_far(job, way, chip, a, v):
        if a + 1 < C - 1:
            @pl.when(left_over(way) >= 3)
            def _():
                relay_on(job, way, chip, a + 1, v).start()

    def spread_near(job, way, chip, a, v, p, owner):
        left = left_over(way)
        if a + 1 < C - 1:
            @pl.when(left == 2)
            def _():
                deliver(job, way, chip, 0, a + 1, v, p, owner).start()

        @pl.when(left >= 1)
        def _():
            deliver(job, way, chip, 0, a, v, p, owner).start()

    far_end = (left_over(0) >= 3) | (left_over(1) >= 3)

    def own_sends():
        def one(p, i):
            for way in range(2):
                @pl.when(can_send(way, 0))
                def _(way=way):
                    line_copy(way, 0, c, p).start()
        loop(0, n1, one)

    def help_far(job):
        lo, n, at, owner = JOBS[job]

        def one(p, i):
            @pl.when(far_end)
            def _():
                enter(p, at + i, owner).wait_recv()
                for way in range(2):
                    spread_far(job, way, c, 0, at + i)
        loop(lo, n, one)

    def help_near(job):
        lo, n, at, owner = JOBS[job]

        def one(p, i):
            @pl.when(jnp.logical_not(far_end))
            def _():
                enter(p, at + i, owner).wait_recv()
            for way in range(2):
                spread_near(job, way, c, 0, at + i, p, owner)
        loop(lo, n, one)

    def help_on(job):
        lo, n, at, owner = JOBS[job]
        for t in range(1, C - 1, 2):
            def one(p, i, t=t):
                v = at + i
                for way in range(2):
                    @pl.when(can_recv(way, t) & (left_over(way) >= 1))
                    def _(way=way):
                        chip = chip_of(way, t)
                        relay_on(job, way, chip, t, v).wait_recv()
                        spread_far(job, way, chip, t + 1, v)
                        spread_near(job, way, chip, t + 1, v, p, owner)
                        deliver(job, way, chip, 1, t, v, p, owner).start()
            loop(lo, n, one)

    def help_direct(job):
        lo, n, at, owner = JOBS[job]

        def one(p, i):
            enter(p, at + i, owner).wait_recv()
            for way in range(2):
                for t in reversed(range(C - 1)):
                    @pl.when(left_over(way) > t)
                    def _(way=way, t=t):
                        deliver(job, way, c, 0, t, at + i, p, owner).start()
        loop(lo, n, one)

    def serve(t):
        def one(p, i):
            for way in range(2):
                @pl.when(can_recv(way, t))
                def _(way=way):
                    chip = chip_of(way, t)
                    line_copy(way, t, chip, p).wait_recv()
                    if t + 1 < C - 1:
                        @pl.when(can_send(way, t + 1))
                        def _():
                            line_copy(way, t + 1, chip, p).start()
                    relay(1 + way * (C - 1) + t, chip, p, True).start()
        loop(0, n1, one)

    def handed(t):
        def one(p, i):
            for way in range(2):
                @pl.when(can_recv(way, t))
                def _(way=way):
                    chip = chip_of(way, t)
                    ref = piece(chip * 2 + core, p)
                    remote(ref, ref, ws.at[0, way, t], ar.at[chip, p], partner).wait_recv()
                    relay(1 + way * (C - 1) + t, chip, p, True).start()
        loop(n1, UNITS - n1, one)

    def enter_all():
        if not shared:
            return
        far = by_role((near[3], 0, 0, 0))

        def one(p, i):
            enter(p, far + i, pair).start()
        loop(n1, by_role(across), one)
        for r, at, step in ((3, 0, -1), (0, across[3], 1)):
            @pl.when(role == r)
            def _(r=r, at=at, step=step):
                def other(p, i):
                    enter(p, at + i, sec + step, 1).start()
                loop(direct[r] + across[r], near[r], other)

    enter_all()

    @pl.when(n0 == 0)
    def _():
        own_sends()
    remote(wall.at[me], wall.at[me], rls.at[0], rlr.at[0], partner).start()
    help_far(0)
    help_near(0)

    def cot_copy(k, j):
        return pltpu.make_async_copy(
            cot_ref.at[k, :, pl.ds(j * CW, CW)], ubuf.at[k, j], uloc.at[k, j])

    @pl.when(sec == S - 1)
    def _():
        for k in range(B):
            for j in range(KH):
                cot_copy(k, j).start()

    for cp in small[1:]:
        cp.wait()
    total = jnp.zeros((B * L, 1), F32)
    for d in range(N):
        xd = x_ref[:, d * w:(d + 1) * w].astype(F32)
        total = total + jnp.sum(xd * xd, axis=-1, keepdims=True)
    inv = lax.rsqrt(total * (1.0 / D) + EPS)
    inv_s[...] = jnp.broadcast_to(inv, inv_s.shape)
    wait_all(gall.at[pl.ds(0, N - 1)], gsem.at[1])
    for d in range(N):
        xd = x_ref[:, d * w:(d + 1) * w].astype(F32)
        ns[d] = (xd * inv * gall[d][0:1, :]).astype(BF16)
        gsh[d] = jnp.zeros(gsh.shape[1:], F32)
    nall[me] = ns[me]
    cos = cos_ref[...]
    sin = sin_ref[...]

    def queries(k, carry):
        rows = pl.ds(pl.multiple_of(k * L, L), L)
        for j in range(KH):
            for g in range(G):
                col = (j * G + g) * HEAD_DIM
                v = ns[col // w, rows, col % w:col % w + HEAD_DIM].astype(F32)
                q = v * cos + pltpu.roll(v, HEAD_DIM // 2, 1) * sin
                qst[k, j, g * L:(g + 1) * L, :] = q.astype(BF16)
        return carry
    lax.fori_loop(0, B, queries, 0)

    def use_step(t):
        for way in range(2):
            @pl.when(can_recv(way, t))
            def _(way=way):
                chip = c - 1 - t if way == 0 else c + 1 + t
                relayed(1 + way * (C - 1) + t, chip, False, rlr)
                acc[...] += dot_nn(ns[chip * 2], wall[chip * 2]) + dot_nn(
                    ns[chip * 2 + 1], wall[chip * 2 + 1])

    help_on(0)

    def send_rows():
        for i in range(1, N):
            peer = (me + i) % N
            remote(ns.at[peer], nall.at[me], nsem.at[0], nsem.at[1], peer).start()

    @pl.when((role == 0) & (n0 > 0) & (NS0 == 0))
    def _():
        send_rows()

    @pl.when(n0 > 0)
    def _():
        own_sends()
    relayed(0, c, False, rlr)
    acc[...] = dot_nn(ns[c * 2], wall[c * 2]) + dot_nn(ns[c * 2 + 1], wall[c * 2 + 1])
    for t in range(C - 1):
        serve(t)
        if t == max(C - 3, 0):
            help_far(1)
        if 0 < t < C - 2:
            handed(t - 1)
    help_near(1)

    @pl.when((role < 3) | (J3T == 0))
    def _():
        help_direct(2)

    @pl.when(((role == 0) & (NS0 == 2)) | ((role == 1) & (NS1 == 2)))
    def _():
        send_rows()

    if C > 2:
        handed(C - 3)
    for t in range(C - 2):
        use_step(t)
    handed(C - 2)
    use_step(C - 2)

    row_pos = lax.broadcasted_iota(jnp.int32, (L, L), 0)
    col_pos = lax.broadcasted_iota(jnp.int32, (L, L), 1)
    causal = (row_pos >= col_pos)[None]

    def attend(k, carry):
        rows = pl.ds(pl.multiple_of(k * L, L), L)
        for j in range(KH):
            kp = acc[rows, j * HEAD_DIM:(j + 1) * HEAD_DIM]
            key = (kp * cos + pltpu.roll(kp, HEAD_DIM // 2, 1) * sin).astype(BF16)
            key_s[k, j] = key
            val_s[k, j] = acc[rows, KV + j * HEAD_DIM:KV + (j + 1) * HEAD_DIM].astype(BF16)
            sc = dot_nt(qst[k, j], key) * scale
            raised = jnp.where(causal, jnp.exp(sc.reshape(G, L, L)), 0.0)
            pr = raised / jnp.sum(raised, axis=-1, keepdims=True)
            prob[k, j] = pr.reshape(G * L, L)
        return carry
    lax.fori_loop(0, B, attend, 0)

    half = C // 2

    def in_turn(outward):
        first = jnp.where(c < half, half - 1 if outward else 0, half if outward else C - 1)
        last = jnp.where(c < half, 0 if outward else half - 1, C - 1 if outward else half)
        away = jnp.where((c < half) == outward, -2, 2)

        @pl.when(c != first)
        def _():
            pl.semaphore_wait(release, 1)

        @pl.when(c != last)
        def _():
            pl.semaphore_signal(
                release, inc=1, device_id=(sec, me + away), device_id_type=MESH)

    @pl.when(((role == 1) & (NS1 == 0)) | ((role == 0) & (NS0 == 1)))
    def _():
        in_turn(False)
        send_rows()

    def usend(k, j):
        return pltpu.make_async_remote_copy(
            src_ref=lowb.at[k, j], dst_ref=ubuf.at[k, j], send_sem=us.at[k, j],
            recv_sem=ur.at[k, j], device_id=(lax.max(sec - 1, 0), me), device_id_type=MESH)

    def kbcopy(k, j, i):
        peer = ((c + i) % C) * 2 + core
        ref = kball.at[me, k, j]
        return remote(ref, ref, kbs.at[k, i], kbr.at[k, i], peer)

    def kbpartner(k, j):
        ref = kball.at[me, k, j]
        return remote(ref, ref, kbs.at[k, 0], kbr.at[k, 0], partner)

    def kbsends(k, j, i):
        right = (i == 1) & (c + 1 < C)
        left = (i == C - 1) & (c >= 1)
        return ((sec == 0) & (KB0 == 1)) | right | left

    def kbshare(k, j):
        kbpartner(k, j).start()
        for i in range(1, C):
            @pl.when(kbsends(k, j, i))
            def _(i=i):
                kbcopy(k, j, i).start()

    def from_chip(way, t):
        return t + 1 if way == 0 else C - 1 - t

    def kbpass(k, way, t):
        ref = kball.at[chip_of(way, t) * 2 + core, k]
        peer = (c + 1 if way == 0 else c - 1) * 2 + core
        return remote(ref, ref, kfs.at[k, way, t], kbr.at[k, from_chip(way, t + 1)], peer)

    def kbrelay(k, i, mine):
        chip = (c - i + C) % C
        ref = kball.at[chip * 2 + (core if mine else 1 - core), k]
        return remote(ref, ref, krs.at[k, i], krr.at[k, i], partner)

    def sent(k):
        @pl.when(sec > 0)
        def _():
            for j in range(KH):
                usend(k, j).wait_send()

    def low_copy(k, j):
        rows = pl.ds(pl.multiple_of(k * L, L), L)
        return pltpu.make_async_copy(
            lowb.at[k, j], low_out.at[rows, pl.ds(j * CW, CW)], lsem.at[k, j])

    def turn(k, carry):
        rows = pl.ds(pl.multiple_of(k * L, L), L)
        keys, values = [], []
        along = jnp.zeros((L, HEAD_DIM), F32)

        @pl.when((k == B - 1) & (role >= 2))
        def _():
            help_on(1)
            if J3T == 1:
                @pl.when(role == 3)
                def _():
                    help_direct(2)
        for j in range(KH):
            @pl.when(sec == S - 1)
            def _(j=j):
                cot_copy(k, j).wait()

            @pl.when(sec < S - 1)
            def _(j=j):
                usend(k, j).wait_recv()
            u = ubuf[k, j]
            us_ = jnp.concatenate(
                [u[:, g * HEAD_DIM:(g + 1) * HEAD_DIM] for g in range(G)], axis=0)
            key, q, pr = key_s[k, j], qst[k, j], prob[k, j]
            gp = dot_nt(us_, val_s[k, j])
            gv = dot_tn(pr.astype(BF16), us_).astype(BF16)
            rd = jnp.sum(pr * gp, axis=-1, keepdims=True)
            gs = (pr * (gp - rd) * scale).astype(BF16)
            gk = dot_tn(gs, q)
            gk = (gk * cos - pltpu.roll(gk, HEAD_DIM // 2, 1) * sin).astype(BF16)
            keys.append(gk)
            values.append(gv)
            kball[me, k, j] = jnp.concatenate([gk, gv], axis=1)
            gq = dot_nn(gs, key)
            at = j * HEAD_DIM
            along = along + gk.astype(F32) * acc[rows, at:at + HEAD_DIM]
            along = along + gv.astype(F32) * acc[rows, KV + at:KV + at + HEAD_DIM]
            for g in range(G):
                v = gq[g * L:(g + 1) * L]
                along = along + v * q[g * L:(g + 1) * L].astype(F32)
                col = (j * G + g) * HEAD_DIM
                gnb[col // w, :, col % w:col % w + HEAD_DIM] = (
                    v * cos - pltpu.roll(v, HEAD_DIM // 2, 1) * sin)
            @pl.when(sec == 0)
            def _(j=j):
                kbshare(k, j)
        @pl.when((sec == S - 1) & (k > 0))
        def _():
            sent(k - 1)
            pl.semaphore_signal(token, inc=1, device_id=(sec, partner), device_id_type=MESH)
        kbv = jnp.concatenate(keys + values, axis=1)
        part_inv = inv_s[rows, 0:1]
        proj = jnp.sum(along, axis=-1, keepdims=True) * (1.0 / D) * part_inv * part_inv
        for j in range(KH):
            for e in range(N // KH):
                d = j * (N // KH) + e
                gn = gnb[d] + dot_nt(kbv, wall[d])
                xd = x_ref[rows, d * w:(d + 1) * w].astype(F32)
                gt = gn * xd * part_inv
                gsh[d] += jnp.sum(gt.reshape(L // 8, 8, w), axis=0)
                u = ubuf[k, j, :, e * w:(e + 1) * w].astype(F32)
                low = (u + part_inv * gall[d][0:1, :] * gn - xd * proj).astype(BF16)
                lowb[k, j, :, e * w:(e + 1) * w] = low
            if j == 0:
                @pl.when((sec == S - 1) & ((k > 0) | (core > 0)))
                def _():
                    pl.semaphore_wait(token, 1)

            low_copy(k, j).start()

            @pl.when(sec > 0)
            def _(j=j):
                usend(k, j).start()
        return carry
    lax.fori_loop(0, B, turn, 0)

    def drained(sem, amounts):
        for r in range(4):
            if amounts[r]:
                @pl.when(role == r)
                def _(r=r):
                    wait_all(wall.at[0, pl.ds(0, amounts[r] * hp)], sem)

    for way in range(2):
        left = left_over(way)
        for t in range(C - 1):
            @pl.when(left > t)
            def _(way=way, t=t):
                drained(hs.at[1, 0, way, t], (0, near[0], 0, across[1]))
        for job, amounts in enumerate((counts, (0, 0, across[0], 0))):
            for a in (0,) + tuple(range(2, C, 2)):
                there = can_recv(way, a - 1) if a else left >= 0
                if a + 1 < C - 1:
                    @pl.when(there & (left >= 3))
                    def _(way=way, a=a, job=job, amounts=amounts):
                        drained(ws.at[1 + job, way, a + 1], amounts)

                    @pl.when(there & (left == 2))
                    def _(way=way, a=a, job=job, amounts=amounts):
                        drained(hs.at[job, 0, way, a + 1], amounts)
                if a < C - 1:
                    @pl.when(there & (left >= 1))
                    def _(way=way, a=a, job=job, amounts=amounts):
                        drained(hs.at[job, 0, way, a], amounts)
                        if a:
                            drained(hs.at[job, 1, way, a - 1], amounts)

    @pl.when(role >= 2)
    def _():
        in_turn(True)

    @pl.when((role >= 2) | ((role == 0) & (n0 == 0) & (NS0 == 0)) | ((role == 1) & (NS1 == 1)))
    def _():
        send_rows()

    @pl.when(sec > 0)
    def _():
        for k in range(B):
            for j in range(KH):
                kbshare(k, j)

    relayed(0, c, True, rls)
    if shared:
        drained(es.at[0], across)
        drained(es.at[1], (near[0], 0, 0, near[3]))
    for t in range(C - 1):
        for way in range(2):
            @pl.when(can_send(way, t) & (can_recv(way, t - 1) if t else True))
            def _(way=way, t=t):
                drained(ws.at[0, way, t], direct)
        for way in range(2):
            @pl.when(can_recv(way, t))
            def _(way=way, t=t):
                relayed(1 + way * (C - 1) + t, chip_of(way, t), True, rls)

    @pl.when((sec == S - 1) & (core == 0))
    def _():
        sent(B - 1)
        pl.semaphore_signal(token, inc=1, device_id=(sec, partner), device_id_type=MESH)

    gsall[me] = gsh[me]
    for i in range(1, N):
        peer = (me + i) % N
        remote(gsh.at[peer], gsall.at[me], ssem.at[0], ssem.at[1], peer).start()
    for k in range(B):
        for t in range(C - 1):
            for way in range(2):
                @pl.when(can_recv(way, t))
                def _(k=k, t=t, way=way):
                    i = from_chip(way, t)
                    wait_all(kball.at[chip_of(way, t) * 2 + core, k], kbr.at[k, i])
                    if t + 1 < C - 1:
                        @pl.when(((sec > 0) | (KB0 == 0)) & can_send(way, t + 1))
                        def _():
                            kbpass(k, way, t).start()
                    kbrelay(k, i, True).start()
    wait_all(nall.at[pl.ds(0, N - 1)], nsem.at[1])
    outs = [pltpu.make_async_copy(nall, rows_out, osem.at[B])]
    outs[0].start()
    for k in range(B):
        wait_all(kball.at[partner, k], kbr.at[k, 0])
        for i in range(1, C):
            kbrelay(k, i, False).wait_recv()
        cp = pltpu.make_async_copy(kball.at[:, k], back_out.at[:, k], osem.at[k])
        cp.start()
        outs.append(cp)
    wait_all(gsall.at[pl.ds(0, N - 1)], ssem.at[1])
    gg = gsall[0]
    for d in range(1, N):
        gg = gg + gsall[d]
    gg_out[...] = jnp.sum(gg, axis=0, keepdims=True)
    for k in range(B):
        for j in range(KH):
            low_copy(k, j).wait()

    wait_all(gall.at[pl.ds(0, N - 1)], gsem.at[0])
    wait_all(nall.at[pl.ds(0, N - 1)], nsem.at[0])
    wait_all(gsall.at[pl.ds(0, N - 1)], ssem.at[0])
    for k in range(B):
        for i in range(C):
            @pl.when(kbsends(k, 0, i) | (i == 0))
            def _(k=k, i=i):
                wait_all(kball.at[me, k], kbs.at[k, i])
            if i:
                kbrelay(k, i, True).wait_send()
        for t in range(C - 2):
            for way in range(2):
                @pl.when(((sec > 0) | (KB0 == 0)) & can_recv(way, t) & can_send(way, t + 1))
                def _(k=k, t=t, way=way):
                    kbpass(k, way, t).wait_send()

    @pl.when(sec < S - 1)
    def _():
        for k in range(B):
            sent(k)

    @pl.when((sec == S - 1) & (core == 1))
    def _():
        sent(B - 1)
    for cp in outs:
        cp.wait()


def finish(plan_ref, low_ref, rows_ref, back_ref, gg_ref, low_out, gk_out, gv_out, gg_out,
           low_s, rows_s, back_s, held, lsem, isem, gsem):
    N, B, KH, L = back_ref.shape[:4]
    w = rows_ref.shape[2]
    fetch_rows = pltpu.make_async_copy(rows_ref, rows_s, isem.at[KH])
    fetch_back = [
        pltpu.make_async_copy(back_ref.at[:, :, j], back_s.at[:, :, j], isem.at[j])
        for j in range(KH)]
    fetch_low = [
        pltpu.make_async_copy(
            low_ref.at[pl.ds(pl.multiple_of(plan_ref[0, k] * L, L), L)], low_s.at[k], lsem.at[0, k])
        for k in range(B)]
    fetch_rows.start()
    for cp in fetch_back + fetch_low:
        cp.start()
    gg_out[...] = gg_ref[...]
    fetch_rows.wait()
    rows_all = rows_s[...].reshape(N * B * L, w)
    copies = []
    for cp in fetch_back:
        cp.wait()
    back = jnp.concatenate([
        jnp.concatenate(
            [back_s[g, k, j, :, i * HEAD_DIM:(i + 1) * HEAD_DIM] for g in range(N) for k in range(B)],
            axis=0)
        for i in range(2) for j in range(KH)], axis=1)
    KV = KH * HEAD_DIM
    part = w // 2
    for half in range(2):
        dw = dot_tn(rows_all[:, half * part:(half + 1) * part], back)
        for i, out in enumerate((gk_out, gv_out)):
            held[i, half * part:(half + 1) * part] = dw[:, i * KV:(i + 1) * KV]
            copies.append(pltpu.make_async_copy(
                held.at[i, pl.ds(half * part, part)], out.at[0, pl.ds(half * part, part)],
                gsem.at[i, half]))
            copies[-1].start()
        if half == 0:
            for k in range(B):
                fetch_low[k].wait()
                copies.append(pltpu.make_async_copy(low_s.at[k], low_out.at[0, k], lsem.at[1, k]))
                copies[-1].start()
    for cp in copies:
        cp.wait()


def body(S, N, inputs, cotangent, norm_gain, key_weight, value_weight, plan):
    B, L, D = inputs.shape[1:]
    w, KV = key_weight.shape[1:]
    KH = KV // HEAD_DIM
    CW = D // KH
    G = CW // HEAD_DIM
    C = N // 2
    slots = line_slots(S, w)
    units = shares(S, w)[0]
    cos, sin = rope_tables(L)
    vmem = pl.BlockSpec(memory_space=pltpu.VMEM)
    hbm = pl.BlockSpec(memory_space=pl.ANY)
    dma = pltpu.SemaphoreType.DMA
    low, rows, back, gg = pl.pallas_call(
        functools.partial(kernel, S, N),
        out_shape=(
            jax.ShapeDtypeStruct((B * L, D), BF16),
            jax.ShapeDtypeStruct((N, B * L, w), BF16),
            jax.ShapeDtypeStruct((N, B, KH, L, 2 * HEAD_DIM), BF16),
            jax.ShapeDtypeStruct((1, w), F32),
        ),
        in_specs=[hbm] * 7,
        out_specs=(hbm, hbm, hbm, vmem),
        scratch_shapes=[
            pltpu.VMEM((B * L, D), BF16),
            pltpu.VMEM((1, w), BF16),
            pltpu.VMEM((L, HEAD_DIM), F32),
            pltpu.VMEM((L, HEAD_DIM), F32),
            pltpu.VMEM((N, w, 2 * KV), BF16),
            pltpu.VMEM((N, B * L, w), BF16),
            pltpu.VMEM((N, B * L, w), BF16),
            pltpu.VMEM((N, 8, w), F32),
            pltpu.VMEM((B * L, 128), F32),
            pltpu.VMEM((B * L, 2 * KV), F32),
            pltpu.VMEM((B, KH, L, HEAD_DIM), BF16),
            pltpu.VMEM((B, KH, L, HEAD_DIM), BF16),
            pltpu.VMEM((B, KH, G * L, HEAD_DIM), BF16),
            pltpu.VMEM((B, KH, G * L, L), F32),
            pltpu.VMEM((B, KH, L, CW), BF16),
            pltpu.VMEM((B, KH, L, CW), BF16),
            pltpu.VMEM((N, L, w), F32),
            pltpu.VMEM((N, B, KH, L, 2 * HEAD_DIM), BF16),
            pltpu.VMEM((N, 8, w), F32),
            pltpu.VMEM((N, 8, w), F32),
            pltpu.VMEM((C, slots, w // units, 2 * KV), BF16),
            dma((6,)),
            dma((3, 2, C - 1)),
            dma((C, slots)),
            dma((2, 2, 2, C - 1)),
            dma((C, units)),
            dma((2,)),
            dma((slots,)),
            pltpu.SemaphoreType.REGULAR,
            pltpu.SemaphoreType.REGULAR,
            dma((2 * C - 1,)),
            dma((2 * C - 1,)),
            dma((2,)),
            dma((2,)),
            dma((2,)),
            dma((B, KH)),
            dma((B, KH)),
            dma((B, KH)),
            dma((B, C)),
            dma((B, C)),
            dma((B, C)),
            dma((B, C)),
            dma((B, 2, max(C - 2, 1))),
            dma((B, KH)),
            dma((B + 1,)),
        ],
        compiler_params=pltpu.CompilerParams(
            collective_id=0, has_side_effects=True, vmem_limit_bytes=56 * 1024 * 1024),
    )(inputs[0].reshape(B * L, D), cotangent, norm_gain, key_weight[0], value_weight[0],
      jnp.asarray(cos), jnp.asarray(sin))
    ordered, gk, gv, gg = pl.pallas_call(
        finish,
        out_shape=(
            jax.ShapeDtypeStruct((1, B, L, D), BF16),
            jax.ShapeDtypeStruct((1, w, KV), F32),
            jax.ShapeDtypeStruct((1, w, KV), F32),
            jax.ShapeDtypeStruct((1, w), F32),
        ),
        in_specs=[pl.BlockSpec(memory_space=pltpu.SMEM), hbm, hbm, hbm, vmem],
        out_specs=(hbm, hbm, hbm, vmem),
        scratch_shapes=[
            pltpu.VMEM((B, L, D), BF16),
            pltpu.VMEM((N, B * L, w), BF16),
            pltpu.VMEM((N, B, KH, L, 2 * HEAD_DIM), BF16),
            pltpu.VMEM((2, w, KV), F32),
            dma((2, B)),
            dma((KH + 1,)),
            dma((2, 2)),
        ],
        compiler_params=pltpu.CompilerParams(vmem_limit_bytes=56 * 1024 * 1024),
    )(plan, low, rows, back, gg)
    return ordered, gk, gv, gg


def solution(mesh):
    in_specs = (
        P("section", None, "dp", None),
        P(None, "dp", None),
        P("section", "dp"),
        P("section", "dp", None),
        P("section", "dp", None),
        P("section", None),
    )
    out_specs = (
        P("section", None, "dp", None),
        P("section", "dp", None),
        P("section", "dp", None),
        P("section", "dp"),
    )
    run = functools.partial(body, mesh.shape["section"], mesh.shape["dp"])
    return jax.shard_map(run, mesh=mesh, in_specs=in_specs, out_specs=out_specs, check_vma=False)
```

```python
import functools
import math

import jax
import jax.numpy as jnp
import numpy as np
from jax import lax
from jax.experimental import pallas as pl
from jax.experimental.pallas import tpu as pltpu
from jax.sharding import PartitionSpec as P

HEAD_DIM = 128
EPS = 1e-05
ROPE_BASE = 500000.0
DIRECT = (9, 13, 8, 10)
ACROSS = (7, 3, 8, 4)
NS0 = 2
NS1 = 2
KB0 = 1
J3T = 0
MESH = pl.DeviceIdType.MESH
F32 = jnp.float32
BF16 = jnp.bfloat16


def dot_nn(a, b):
    return lax.dot_general(a, b, (((1,), (0,)), ((), ())), preferred_element_type=F32)


def dot_nt(a, b):
    return lax.dot_general(a, b, (((1,), (1,)), ((), ())), preferred_element_type=F32)


def dot_tn(a, b):
    return lax.dot_general(a, b, (((0,), (0,)), ((), ())), preferred_element_type=F32)


def rope_tables(length):
    half = HEAD_DIM // 2
    freq = (ROPE_BASE ** (-(np.arange(half, dtype=np.float32) * 2.0 / HEAD_DIM))).astype(np.float32)
    angles = np.arange(length, dtype=np.float32)[:, None] * freq[None, :]
    cos, sin = np.cos(angles), np.sin(angles)
    return (
        np.concatenate([cos, cos], -1).astype(np.float32),
        np.concatenate([-sin, sin], -1).astype(np.float32),
    )


def shares(S, w):
    units = 16 if w % 256 == 0 else 8
    if S % 4:
        return units, False, (units,) * 4, (0,) * 4, (0,) * 4
    direct = tuple(d * units // 16 for d in DIRECT)
    across = tuple(a * units // 16 if r % 3 == 0 else units - direct[r] for r, a in enumerate(ACROSS))
    return units, True, direct, across, tuple(units - d - a for d, a in zip(direct, across))


def line_slots(S, w):
    units, shared, direct, across, near = shares(S, w)
    before = (across[2], across[3], near[3], 0)
    after = (0, near[0], across[0], across[1])
    return max(1, max(before[r] + after[r] for r in range(4)))


def kernel(S, N, x_hbm, cot_ref, gain_hbm, wk_ref, wv_ref, cos_hbm, sin_hbm,
           low_out, rows_out, back_out, gg_out,
           x_ref, gain_ref, cos_ref, sin_ref, wall, ns, nall, gall, inv_s, acc, key_s, val_s, qst, prob, ubuf, lowb, gnb,
           kball, gsh, gsum, gsall, stage,
           loc, ws, wr, hs, ar, es, er, token, release, rls, rlr, gsem, nsem, ssem, us, ur, uloc, kbs, kbr, krs, krr, kfs, lsem, osem):
    B, KH, L = ubuf.shape[0], ubuf.shape[1], ubuf.shape[2]
    CW = ubuf.shape[3]
    w = wall.shape[1]
    KV = KH * HEAD_DIM
    G = CW // HEAD_DIM
    D = x_ref.shape[1]
    C = N // 2
    scale = 1.0 / math.sqrt(HEAD_DIM)
    sec = lax.axis_index("section")
    me = lax.axis_index("dp")
    c = me // 2
    core = me % 2
    partner = c * 2 + (1 - core)
    role = sec % 4
    UNITS, shared, direct, across, near = shares(S, w)
    hp = w // UNITS

    def by_role(values):
        out = jnp.int32(values[3])
        for r in range(3):
            out = jnp.where(role == r, jnp.int32(values[r]), out)
        return out

    up = role >= 2
    pair = jnp.where(up, sec - 2, sec + 2) if shared else sec
    first = (direct[2], direct[3], direct[3] + across[3], 0)
    counts = (across[2], across[3], near[3], 0)
    lo0, n0 = by_role(first), by_role(counts)
    n1 = by_role(direct)
    n2 = by_role((0, 0, across[0], 0))
    n3 = by_role((0, near[0], 0, across[1]))
    lo3 = by_role((0, direct[0] + across[0], 0, direct[1]))
    owner3 = jnp.where(role == 1, sec - 1, pair)
    owner0 = jnp.where(role == 2, sec + 1, pair)

    def remote(src, dst, send, recv, peer):
        return pltpu.make_async_remote_copy(
            src_ref=src, dst_ref=dst, send_sem=send, recv_sem=recv,
            device_id=(sec, peer), device_id_type=MESH)

    def wait_all(ref, sem):
        pltpu.make_async_copy(ref, ref, sem).wait()

    ck = pltpu.make_async_copy(wk_ref, wall.at[me, :, pl.ds(0, KV)], loc.at[0])
    cv = pltpu.make_async_copy(wv_ref, wall.at[me, :, pl.ds(KV, KV)], loc.at[1])
    small = [
        pltpu.make_async_copy(src, dst, loc.at[2 + i])
        for i, (src, dst) in enumerate((
            (gain_hbm, gain_ref), (x_hbm, x_ref), (cos_hbm, cos_ref), (sin_hbm, sin_ref)))]
    small[0].start()
    ck.start()
    cv.start()
    for cp in small[1:]:
        cp.start()

    barrier = pltpu.get_barrier_semaphore()
    for i in range(1, N):
        pl.semaphore_signal(barrier, inc=1, device_id=(sec, (me + i) % N), device_id_type=MESH)

    @pl.when(sec > 0)
    def _():
        pl.semaphore_signal(barrier, inc=1, device_id=(sec - 1, me), device_id_type=MESH)

    @pl.when(sec < S - 1)
    def _():
        pl.semaphore_signal(barrier, inc=1, device_id=(sec + 1, me), device_id_type=MESH)
    if shared:
        first_sec = sec - role
        for step in range(1, 4):
            for i in range(C):
                pl.semaphore_signal(
                    barrier, inc=1, device_id=(first_sec + (role + step) % 4, i * 2 + core),
                    device_id_type=MESH)
    below = jnp.where(sec > 0, 1, 0)
    above = jnp.where(sec < S - 1, 1, 0)
    pl.semaphore_wait(barrier, N - 1 + below + above + (3 * C if shared else 0))

    small[0].wait()
    gall[me] = jnp.broadcast_to(gain_ref[...].astype(F32), gall.shape[1:])
    gcopies = []
    for i in range(1, N):
        cp = remote(gall.at[me], gall.at[me], gsem.at[0], gsem.at[1], (me + i) % N)
        cp.start()
        gcopies.append(cp)
    ck.wait()
    cv.wait()

    def piece(shard, p):
        return wall.at[shard, pl.ds(p * hp, hp)]

    def chip_of(way, t):
        return c - 1 - t if way == 0 else c + 1 + t

    def line_copy(way, t, chip, p):
        peer = (c + 1 if way == 0 else c - 1) * 2 + core
        ref = piece(chip * 2 + core, p)
        return remote(ref, ref, ws.at[0, way, t], ar.at[chip, p], peer)

    def relay(slot, chip, p, mine):
        ref = piece(chip * 2 + (core if mine else 1 - core), p)
        return remote(ref, ref, rls.at[slot], rlr.at[slot], partner)

    def relayed(slot, chip, mine, sem):
        wait_all(wall.at[chip * 2 + (core if mine else 1 - core)], sem.at[slot])

    def enter(p, v, helper, kind=0):
        return pltpu.make_async_remote_copy(
            src_ref=piece(me, p), dst_ref=stage.at[c, v], send_sem=es.at[kind],
            recv_sem=er.at[v], device_id=(helper, me), device_id_type=MESH)

    def deliver(job, way, chip, kind, t, v, p, owner):
        peer = (chip + t + 1 if way == 0 else chip - t - 1) * 2 + core
        return pltpu.make_async_remote_copy(
            src_ref=stage.at[chip, v], dst_ref=piece(chip * 2 + core, p),
            send_sem=hs.at[min(job, 1), kind, way, t], recv_sem=ar.at[chip, p],
            device_id=(owner, peer), device_id_type=MESH)

    def relay_on(job, way, chip, t, v):
        peer = (chip + t + 1 if way == 0 else chip - t - 1) * 2 + core
        ref = stage.at[chip, v]
        return remote(ref, ref, ws.at[1 + job, way, t], wr.at[chip, v], peer)

    def can_send(way, t):
        return ((c - t >= 0) & (c + 1 < C)) if way == 0 else ((c + t < C) & (c >= 1))

    def can_recv(way, t):
        return (c - 1 - t >= 0) if way == 0 else (c + 1 + t < C)

    def loop(lo, n, f):
        def step(i, carry):
            f(lo + i, i)
            return carry
        lax.fori_loop(0, n, step, 0)

    JOBS = (
        (lo0, n0, 0, owner0),
        (direct[0], n2, n0, pair),
        (lo3, n3, n0, owner3),
    )

    def left_over(way):
        return C - 1 - c if way == 0 else c

    def spread_far(job, way, chip, a, v):
        if a + 1 < C - 1:
            @pl.when(left_over(way) >= 3)
            def _():
                relay_on(job, way, chip, a + 1, v).start()

    def spread_near(job, way, chip, a, v, p, owner):
        left = left_over(way)
        if a + 1 < C - 1:
            @pl.when(left == 2)
            def _():
                deliver(job, way, chip, 0, a + 1, v, p, owner).start()

        @pl.when(left >= 1)
        def _():
            deliver(job, way, chip, 0, a, v, p, owner).start()

    far_end = (left_over(0) >= 3) | (left_over(1) >= 3)

    def own_sends():
        def one(p, i):
            for way in range(2):
                @pl.when(can_send(way, 0))
                def _(way=way):
                    line_copy(way, 0, c, p).start()
        loop(0, n1, one)

    def help_far(job):
        lo, n, at, owner = JOBS[job]

        def one(p, i):
            @pl.when(far_end)
            def _():
                enter(p, at + i, owner).wait_recv()
                for way in range(2):
                    spread_far(job, way, c, 0, at + i)
        loop(lo, n, one)

    def help_near(job):
        lo, n, at, owner = JOBS[job]

        def one(p, i):
            @pl.when(jnp.logical_not(far_end))
            def _():
                enter(p, at + i, owner).wait_recv()
            for way in range(2):
                spread_near(job, way, c, 0, at + i, p, owner)
        loop(lo, n, one)

    def help_on(job):
        lo, n, at, owner = JOBS[job]
        for t in range(1, C - 1, 2):
            def one(p, i, t=t):
                v = at + i
                for way in range(2):
                    @pl.when(can_recv(way, t) & (left_over(way) >= 1))
                    def _(way=way):
                        chip = chip_of(way, t)
                        relay_on(job, way, chip, t, v).wait_recv()
                        spread_far(job, way, chip, t + 1, v)
                        spread_near(job, way, chip, t + 1, v, p, owner)
                        deliver(job, way, chip, 1, t, v, p, owner).start()
            loop(lo, n, one)

    def help_direct(job):
        lo, n, at, owner = JOBS[job]

        def one(p, i):
            enter(p, at + i, owner).wait_recv()
            for way in range(2):
                for t in reversed(range(C - 1)):
                    @pl.when(left_over(way) > t)
                    def _(way=way, t=t):
                        deliver(job, way, c, 0, t, at + i, p, owner).start()
        loop(lo, n, one)

    def serve(t):
        def one(p, i):
            for way in range(2):
                @pl.when(can_recv(way, t))
                def _(way=way):
                    chip = chip_of(way, t)
                    line_copy(way, t, chip, p).wait_recv()
                    if t + 1 < C - 1:
                        @pl.when(can_send(way, t + 1))
                        def _():
                            line_copy(way, t + 1, chip, p).start()
                    relay(1 + way * (C - 1) + t, chip, p, True).start()
        loop(0, n1, one)

    def handed(t):
        def one(p, i):
            for way in range(2):
                @pl.when(can_recv(way, t))
                def _(way=way):
                    chip = chip_of(way, t)
                    ref = piece(chip * 2 + core, p)
                    remote(ref, ref, ws.at[0, way, t], ar.at[chip, p], partner).wait_recv()
                    relay(1 + way * (C - 1) + t, chip, p, True).start()
        loop(n1, UNITS - n1, one)

    def enter_all():
        if not shared:
            return
        far = by_role((near[3], 0, 0, 0))

        def one(p, i):
            enter(p, far + i, pair).start()
        loop(n1, by_role(across), one)
        for r, at, step in ((3, 0, -1), (0, across[3], 1)):
            @pl.when(role == r)
            def _(r=r, at=at, step=step):
                def other(p, i):
                    enter(p, at + i, sec + step, 1).start()
                loop(direct[r] + across[r], near[r], other)

    enter_all()

    @pl.when(n0 == 0)
    def _():
        own_sends()
    remote(wall.at[me], wall.at[me], rls.at[0], rlr.at[0], partner).start()
    help_far(0)
    help_near(0)

    def cot_copy(k, j):
        return pltpu.make_async_copy(
            cot_ref.at[k, :, pl.ds(j * CW, CW)], ubuf.at[k, j], uloc.at[k, j])

    @pl.when(sec == S - 1)
    def _():
        for k in range(B):
            for j in range(KH):
                cot_copy(k, j).start()

    for cp in small[1:]:
        cp.wait()
    total = jnp.zeros((B * L, 1), F32)
    for d in range(N):
        xd = x_ref[:, d * w:(d + 1) * w].astype(F32)
        total = total + jnp.sum(xd * xd, axis=-1, keepdims=True)
    inv = lax.rsqrt(total * (1.0 / D) + EPS)
    inv_s[...] = jnp.broadcast_to(inv, inv_s.shape)
    wait_all(gall.at[pl.ds(0, N - 1)], gsem.at[1])
    for d in range(N):
        xd = x_ref[:, d * w:(d + 1) * w].astype(F32)
        ns[d] = (xd * inv * gall[d][0:1, :]).astype(BF16)
        gsh[d] = jnp.zeros(gsh.shape[1:], F32)
    nall[me] = ns[me]
    cos = cos_ref[...]
    sin = sin_ref[...]

    def queries(k, carry):
        rows = pl.ds(pl.multiple_of(k * L, L), L)
        for j in range(KH):
            for g in range(G):
                col = (j * G + g) * HEAD_DIM
                v = ns[col // w, rows, col % w:col % w + HEAD_DIM].astype(F32)
                q = v * cos + pltpu.roll(v, HEAD_DIM // 2, 1) * sin
                qst[k, j, g * L:(g + 1) * L, :] = q.astype(BF16)
        return carry
    lax.fori_loop(0, B, queries, 0)

    def use_step(t):
        for way in range(2):
            @pl.when(can_recv(way, t))
            def _(way=way):
                chip = c - 1 - t if way == 0 else c + 1 + t
                relayed(1 + way * (C - 1) + t, chip, False, rlr)
                acc[...] += dot_nn(ns[chip * 2], wall[chip * 2]) + dot_nn(
                    ns[chip * 2 + 1], wall[chip * 2 + 1])

    help_on(0)

    def send_rows():
        for i in range(1, N):
            peer = (me + i) % N
            remote(ns.at[peer], nall.at[me], nsem.at[0], nsem.at[1], peer).start()

    @pl.when((role == 0) & (n0 > 0) & (NS0 == 0))
    def _():
        send_rows()

    @pl.when(n0 > 0)
    def _():
        own_sends()
    relayed(0, c, False, rlr)
    acc[...] = dot_nn(ns[c * 2], wall[c * 2]) + dot_nn(ns[c * 2 + 1], wall[c * 2 + 1])
    for t in range(C - 1):
        serve(t)
        if t == max(C - 3, 0):
            help_far(1)
        if 0 < t < C - 2:
            handed(t - 1)
    help_near(1)

    @pl.when((role < 3) | (J3T == 0))
    def _():
        help_direct(2)

    @pl.when(((role == 0) & (NS0 == 2)) | ((role == 1) & (NS1 == 2)))
    def _():
        send_rows()

    if C > 2:
        handed(C - 3)
    for t in range(C - 2):
        use_step(t)
    handed(C - 2)
    use_step(C - 2)

    row_pos = lax.broadcasted_iota(jnp.int32, (L, L), 0)
    col_pos = lax.broadcasted_iota(jnp.int32, (L, L), 1)
    causal = (row_pos >= col_pos)[None]

    def attend(k, carry):
        rows = pl.ds(pl.multiple_of(k * L, L), L)
        for j in range(KH):
            kp = acc[rows, j * HEAD_DIM:(j + 1) * HEAD_DIM]
            key = (kp * cos + pltpu.roll(kp, HEAD_DIM // 2, 1) * sin).astype(BF16)
            key_s[k, j] = key
            val_s[k, j] = acc[rows, KV + j * HEAD_DIM:KV + (j + 1) * HEAD_DIM].astype(BF16)
            sc = dot_nt(qst[k, j], key) * scale
            raised = jnp.where(causal, jnp.exp(sc.reshape(G, L, L)), 0.0)
            pr = raised / jnp.sum(raised, axis=-1, keepdims=True)
            prob[k, j] = pr.reshape(G * L, L)
        return carry
    lax.fori_loop(0, B, attend, 0)

    half = C // 2

    def in_turn(outward):
        first = jnp.where(c < half, half - 1 if outward else 0, half if outward else C - 1)
        last = jnp.where(c < half, 0 if outward else half - 1, C - 1 if outward else half)
        away = jnp.where((c < half) == outward, -2, 2)

        @pl.when(c != first)
        def _():
            pl.semaphore_wait(release, 1)

        @pl.when(c != last)
        def _():
            pl.semaphore_signal(
                release, inc=1, device_id=(sec, me + away), device_id_type=MESH)

    @pl.when(((role == 1) & (NS1 == 0)) | ((role == 0) & (NS0 == 1)))
    def _():
        in_turn(False)
        send_rows()

    def usend(k, j):
        return pltpu.make_async_remote_copy(
            src_ref=lowb.at[k, j], dst_ref=ubuf.at[k, j], send_sem=us.at[k, j],
            recv_sem=ur.at[k, j], device_id=(lax.max(sec - 1, 0), me), device_id_type=MESH)

    def kbcopy(k, j, i):
        peer = ((c + i) % C) * 2 + core
        ref = kball.at[me, k, j]
        return remote(ref, ref, kbs.at[k, i], kbr.at[k, i], peer)

    def kbpartner(k, j):
        ref = kball.at[me, k, j]
        return remote(ref, ref, kbs.at[k, 0], kbr.at[k, 0], partner)

    def kbsends(k, j, i):
        right = (i == 1) & (c + 1 < C)
        left = (i == C - 1) & (c >= 1)
        return ((sec == 0) & (KB0 == 1)) | right | left

    def kbshare(k, j):
        kbpartner(k, j).start()
        for i in range(1, C):
            @pl.when(kbsends(k, j, i))
            def _(i=i):
                kbcopy(k, j, i).start()

    def from_chip(way, t):
        return t + 1 if way == 0 else C - 1 - t

    def kbpass(k, way, t):
        ref = kball.at[chip_of(way, t) * 2 + core, k]
        peer = (c + 1 if way == 0 else c - 1) * 2 + core
        return remote(ref, ref, kfs.at[k, way, t], kbr.at[k, from_chip(way, t + 1)], peer)

    def kbrelay(k, i, mine):
        chip = (c - i + C) % C
        ref = kball.at[chip * 2 + (core if mine else 1 - core), k]
        return remote(ref, ref, krs.at[k, i], krr.at[k, i], partner)

    def sent(k):
        @pl.when(sec > 0)
        def _():
            for j in range(KH):
                usend(k, j).wait_send()

    def low_copy(k, j):
        rows = pl.ds(pl.multiple_of(k * L, L), L)
        return pltpu.make_async_copy(
            lowb.at[k, j], low_out.at[rows, pl.ds(j * CW, CW)], lsem.at[k, j])

    def turn(k, carry):
        rows = pl.ds(pl.multiple_of(k * L, L), L)
        keys, values = [], []
        along = jnp.zeros((L, HEAD_DIM), F32)

        @pl.when((k == B - 1) & (role >= 2))
        def _():
            help_on(1)
            if J3T == 1:
                @pl.when(role == 3)
                def _():
                    help_direct(2)
        for j in range(KH):
            @pl.when(sec == S - 1)
            def _(j=j):
                cot_copy(k, j).wait()

            @pl.when(sec < S - 1)
            def _(j=j):
                usend(k, j).wait_recv()
            u = ubuf[k, j]
            us_ = jnp.concatenate(
                [u[:, g * HEAD_DIM:(g + 1) * HEAD_DIM] for g in range(G)], axis=0)
            key, q, pr = key_s[k, j], qst[k, j], prob[k, j]
            gp = dot_nt(us_, val_s[k, j])
            gv = dot_tn(pr.astype(BF16), us_).astype(BF16)
            rd = jnp.sum(pr * gp, axis=-1, keepdims=True)
            gs = (pr * (gp - rd) * scale).astype(BF16)
            gk = dot_tn(gs, q)
            gk = (gk * cos - pltpu.roll(gk, HEAD_DIM // 2, 1) * sin).astype(BF16)
            keys.append(gk)
            values.append(gv)
            kball[me, k, j] = jnp.concatenate([gk, gv], axis=1)
            gq = dot_nn(gs, key)
            at = j * HEAD_DIM
            along = along + gk.astype(F32) * acc[rows, at:at + HEAD_DIM]
            along = along + gv.astype(F32) * acc[rows, KV + at:KV + at + HEAD_DIM]
            for g in range(G):
                v = gq[g * L:(g + 1) * L]
                along = along + v * q[g * L:(g + 1) * L].astype(F32)
                col = (j * G + g) * HEAD_DIM
                gnb[col // w, :, col % w:col % w + HEAD_DIM] = (
                    v * cos - pltpu.roll(v, HEAD_DIM // 2, 1) * sin)
            @pl.when(sec == 0)
            def _(j=j):
                kbshare(k, j)
        @pl.when((sec == S - 1) & (k > 0))
        def _():
            sent(k - 1)
            pl.semaphore_signal(token, inc=1, device_id=(sec, partner), device_id_type=MESH)
        kbv = jnp.concatenate(keys + values, axis=1)
        part_inv = inv_s[rows, 0:1]
        proj = jnp.sum(along, axis=-1, keepdims=True) * (1.0 / D) * part_inv * part_inv
        for j in range(KH):
            for e in range(N // KH):
                d = j * (N // KH) + e
                gn = gnb[d] + dot_nt(kbv, wall[d])
                xd = x_ref[rows, d * w:(d + 1) * w].astype(F32)
                gt = gn * xd * part_inv
                gsh[d] += jnp.sum(gt.reshape(L // 8, 8, w), axis=0)
                u = ubuf[k, j, :, e * w:(e + 1) * w].astype(F32)
                low = (u + part_inv * gall[d][0:1, :] * gn - xd * proj).astype(BF16)
                lowb[k, j, :, e * w:(e + 1) * w] = low
            if j == 0:
                @pl.when((sec == S - 1) & ((k > 0) | (core > 0)))
                def _():
                    pl.semaphore_wait(token, 1)

            low_copy(k, j).start()

            @pl.when(sec > 0)
            def _(j=j):
                usend(k, j).start()
        return carry
    lax.fori_loop(0, B, turn, 0)

    def drained(sem, amounts):
        for r in range(4):
            if amounts[r]:
                @pl.when(role == r)
                def _(r=r):
                    wait_all(wall.at[0, pl.ds(0, amounts[r] * hp)], sem)

    for way in range(2):
        left = left_over(way)
        for t in range(C - 1):
            @pl.when(left > t)
            def _(way=way, t=t):
                drained(hs.at[1, 0, way, t], (0, near[0], 0, across[1]))
        for job, amounts in enumerate((counts, (0, 0, across[0], 0))):
            for a in (0,) + tuple(range(2, C, 2)):
                there = can_recv(way, a - 1) if a else left >= 0
                if a + 1 < C - 1:
                    @pl.when(there & (left >= 3))
                    def _(way=way, a=a, job=job, amounts=amounts):
                        drained(ws.at[1 + job, way, a + 1], amounts)

                    @pl.when(there & (left == 2))
                    def _(way=way, a=a, job=job, amounts=amounts):
                        drained(hs.at[job, 0, way, a + 1], amounts)
                if a < C - 1:
                    @pl.when(there & (left >= 1))
                    def _(way=way, a=a, job=job, amounts=amounts):
                        drained(hs.at[job, 0, way, a], amounts)
                        if a:
                            drained(hs.at[job, 1, way, a - 1], amounts)

    @pl.when(role >= 2)
    def _():
        in_turn(True)

    @pl.when((role >= 2) | ((role == 0) & (n0 == 0) & (NS0 == 0)) | ((role == 1) & (NS1 == 1)))
    def _():
        send_rows()

    @pl.when(sec > 0)
    def _():
        for k in range(B):
            for j in range(KH):
                kbshare(k, j)

    relayed(0, c, True, rls)
    if shared:
        drained(es.at[0], across)
        drained(es.at[1], (near[0], 0, 0, near[3]))
    for t in range(C - 1):
        for way in range(2):
            @pl.when(can_send(way, t) & (can_recv(way, t - 1) if t else True))
            def _(way=way, t=t):
                drained(ws.at[0, way, t], direct)
        for way in range(2):
            @pl.when(can_recv(way, t))
            def _(way=way, t=t):
                relayed(1 + way * (C - 1) + t, chip_of(way, t), True, rls)

    @pl.when((sec == S - 1) & (core == 0))
    def _():
        sent(B - 1)
        pl.semaphore_signal(token, inc=1, device_id=(sec, partner), device_id_type=MESH)

    for d in range(N):
        gsum[d] = jnp.sum(gsh[d], axis=0, keepdims=True)
    gsall[me] = gsum[me]
    for i in range(1, N):
        peer = (me + i) % N
        remote(gsum.at[peer], gsall.at[me], ssem.at[0], ssem.at[1], peer).start()
    for k in range(B):
        for t in range(C - 1):
            for way in range(2):
                @pl.when(can_recv(way, t))
                def _(k=k, t=t, way=way):
                    i = from_chip(way, t)
                    wait_all(kball.at[chip_of(way, t) * 2 + core, k], kbr.at[k, i])
                    if t + 1 < C - 1:
                        @pl.when(((sec > 0) | (KB0 == 0)) & can_send(way, t + 1))
                        def _():
                            kbpass(k, way, t).start()
                    kbrelay(k, i, True).start()
    wait_all(nall.at[pl.ds(0, N - 1)], nsem.at[1])
    outs = [pltpu.make_async_copy(nall, rows_out, osem.at[B])]
    outs[0].start()
    for k in range(B):
        wait_all(kball.at[partner, k], kbr.at[k, 0])
        for i in range(1, C):
            kbrelay(k, i, False).wait_recv()
        cp = pltpu.make_async_copy(kball.at[:, k], back_out.at[:, k], osem.at[k])
        cp.start()
        outs.append(cp)
    wait_all(gsall.at[pl.ds(0, N - 1)], ssem.at[1])
    gg = gsall[0]
    for d in range(1, N):
        gg = gg + gsall[d]
    gg_out[...] = gg
    for k in range(B):
        for j in range(KH):
            low_copy(k, j).wait()

    wait_all(gall.at[pl.ds(0, N - 1)], gsem.at[0])
    wait_all(nall.at[pl.ds(0, N - 1)], nsem.at[0])
    wait_all(gsall.at[pl.ds(0, N - 1)], ssem.at[0])
    for k in range(B):
        for i in range(C):
            @pl.when(kbsends(k, 0, i) | (i == 0))
            def _(k=k, i=i):
                wait_all(kball.at[me, k], kbs.at[k, i])
            if i:
                kbrelay(k, i, True).wait_send()
        for t in range(C - 2):
            for way in range(2):
                @pl.when(((sec > 0) | (KB0 == 0)) & can_recv(way, t) & can_send(way, t + 1))
                def _(k=k, t=t, way=way):
                    kbpass(k, way, t).wait_send()

    @pl.when(sec < S - 1)
    def _():
        for k in range(B):
            sent(k)

    @pl.when((sec == S - 1) & (core == 1))
    def _():
        sent(B - 1)
    for cp in outs:
        cp.wait()


def finish(plan_ref, low_ref, rows_ref, back_ref, gg_ref, low_out, gk_out, gv_out, gg_out,
           low_s, rows_s, back_s, held, lsem, isem, gsem):
    N, B, KH, L = back_ref.shape[:4]
    w = rows_ref.shape[2]
    fetch_rows = pltpu.make_async_copy(rows_ref, rows_s, isem.at[KH])
    fetch_back = [
        pltpu.make_async_copy(back_ref.at[:, :, j], back_s.at[:, :, j], isem.at[j])
        for j in range(KH)]
    fetch_low = [
        pltpu.make_async_copy(
            low_ref.at[pl.ds(pl.multiple_of(plan_ref[0, k] * L, L), L)], low_s.at[k], lsem.at[0, k])
        for k in range(B)]
    fetch_rows.start()
    for cp in fetch_back:
        cp.start()
    gg_out[...] = gg_ref[...]
    fetch_rows.wait()
    rows_all = rows_s[...].reshape(N * B * L, w)
    copies = []
    for cp in fetch_back:
        cp.wait()
    for cp in fetch_low:
        cp.start()
    back = jnp.concatenate([
        jnp.concatenate(
            [back_s[g, k, j, :, i * HEAD_DIM:(i + 1) * HEAD_DIM] for g in range(N) for k in range(B)],
            axis=0)
        for i in range(2) for j in range(KH)], axis=1)
    KV = KH * HEAD_DIM
    part = w // 2
    for half in range(2):
        dw = dot_tn(rows_all[:, half * part:(half + 1) * part], back)
        for i, out in enumerate((gk_out, gv_out)):
            held[i, half * part:(half + 1) * part] = dw[:, i * KV:(i + 1) * KV]
            copies.append(pltpu.make_async_copy(
                held.at[i, pl.ds(half * part, part)], out.at[0, pl.ds(half * part, part)],
                gsem.at[i, half]))
            copies[-1].start()
        if half == 0:
            for k in range(B):
                fetch_low[k].wait()
                copies.append(pltpu.make_async_copy(low_s.at[k], low_out.at[0, k], lsem.at[1, k]))
                copies[-1].start()
    for cp in copies:
        cp.wait()


def body(S, N, inputs, cotangent, norm_gain, key_weight, value_weight, plan):
    B, L, D = inputs.shape[1:]
    w, KV = key_weight.shape[1:]
    KH = KV // HEAD_DIM
    CW = D // KH
    G = CW // HEAD_DIM
    C = N // 2
    slots = line_slots(S, w)
    units = shares(S, w)[0]
    cos, sin = rope_tables(L)
    vmem = pl.BlockSpec(memory_space=pltpu.VMEM)
    hbm = pl.BlockSpec(memory_space=pl.ANY)
    dma = pltpu.SemaphoreType.DMA
    low, rows, back, gg = pl.pallas_call(
        functools.partial(kernel, S, N),
        out_shape=(
            jax.ShapeDtypeStruct((B * L, D), BF16),
            jax.ShapeDtypeStruct((N, B * L, w), BF16),
            jax.ShapeDtypeStruct((N, B, KH, L, 2 * HEAD_DIM), BF16),
            jax.ShapeDtypeStruct((1, w), F32),
        ),
        in_specs=[hbm] * 7,
        out_specs=(hbm, hbm, hbm, vmem),
        scratch_shapes=[
            pltpu.VMEM((B * L, D), BF16),
            pltpu.VMEM((1, w), BF16),
            pltpu.VMEM((L, HEAD_DIM), F32),
            pltpu.VMEM((L, HEAD_DIM), F32),
            pltpu.VMEM((N, w, 2 * KV), BF16),
            pltpu.VMEM((N, B * L, w), BF16),
            pltpu.VMEM((N, B * L, w), BF16),
            pltpu.VMEM((N, 8, w), F32),
            pltpu.VMEM((B * L, 128), F32),
            pltpu.VMEM((B * L, 2 * KV), F32),
            pltpu.VMEM((B, KH, L, HEAD_DIM), BF16),
            pltpu.VMEM((B, KH, L, HEAD_DIM), BF16),
            pltpu.VMEM((B, KH, G * L, HEAD_DIM), BF16),
            pltpu.VMEM((B, KH, G * L, L), F32),
            pltpu.VMEM((B, KH, L, CW), BF16),
            pltpu.VMEM((B, KH, L, CW), BF16),
            pltpu.VMEM((N, L, w), F32),
            pltpu.VMEM((N, B, KH, L, 2 * HEAD_DIM), BF16),
            pltpu.VMEM((N, 8, w), F32),
            pltpu.VMEM((N, 1, w), F32),
            pltpu.VMEM((N, 1, w), F32),
            pltpu.VMEM((C, slots, w // units, 2 * KV), BF16),
            dma((6,)),
            dma((3, 2, C - 1)),
            dma((C, slots)),
            dma((2, 2, 2, C - 1)),
            dma((C, units)),
            dma((2,)),
            dma((slots,)),
            pltpu.SemaphoreType.REGULAR,
            pltpu.SemaphoreType.REGULAR,
            dma((2 * C - 1,)),
            dma((2 * C - 1,)),
            dma((2,)),
            dma((2,)),
            dma((2,)),
            dma((B, KH)),
            dma((B, KH)),
            dma((B, KH)),
            dma((B, C)),
            dma((B, C)),
            dma((B, C)),
            dma((B, C)),
            dma((B, 2, max(C - 2, 1))),
            dma((B, KH)),
            dma((B + 1,)),
        ],
        compiler_params=pltpu.CompilerParams(
            collective_id=0, has_side_effects=True, vmem_limit_bytes=56 * 1024 * 1024),
    )(inputs[0].reshape(B * L, D), cotangent, norm_gain, key_weight[0], value_weight[0],
      jnp.asarray(cos), jnp.asarray(sin))
    ordered, gk, gv, gg = pl.pallas_call(
        finish,
        out_shape=(
            jax.ShapeDtypeStruct((1, B, L, D), BF16),
            jax.ShapeDtypeStruct((1, w, KV), F32),
            jax.ShapeDtypeStruct((1, w, KV), F32),
            jax.ShapeDtypeStruct((1, w), F32),
        ),
        in_specs=[pl.BlockSpec(memory_space=pltpu.SMEM), hbm, hbm, hbm, vmem],
        out_specs=(hbm, hbm, hbm, vmem),
        scratch_shapes=[
            pltpu.VMEM((B, L, D), BF16),
            pltpu.VMEM((N, B * L, w), BF16),
            pltpu.VMEM((N, B, KH, L, 2 * HEAD_DIM), BF16),
            pltpu.VMEM((2, w, KV), F32),
            dma((2, B)),
            dma((KH + 1,)),
            dma((2, 2)),
        ],
        compiler_params=pltpu.CompilerParams(vmem_limit_bytes=56 * 1024 * 1024),
    )(plan, low, rows, back, gg)
    return ordered, gk, gv, gg


def solution(mesh):
    in_specs = (
        P("section", None, "dp", None),
        P(None, "dp", None),
        P("section", "dp"),
        P("section", "dp", None),
        P("section", "dp", None),
        P("section", None),
    )
    out_specs = (
        P("section", None, "dp", None),
        P("section", "dp", None),
        P("section", "dp", None),
        P("section", "dp"),
    )
    run = functools.partial(body, mesh.shape["section"], mesh.shape["dp"])
    return jax.shard_map(run, mesh=mesh, in_specs=in_specs, out_specs=out_specs, check_vma=False)
```
